128 devices in a mesh: sec: 64 (over x, y, z), node: 2 (over core).
Axes of the slice: x: 4, y: 4, z: 4, core: 2. Of those that a mesh axis runs over, the one named last changes fastest.
Arguments:
- env_blocks: bfloat16 [2, 24576, 128, 128], P('node', 'sec'), may hold values from -10 to 10, as said below
- iso_blocks: bfloat16 [2, 24576, 128, 128], P('node', 'sec'), may hold values from -6 to 6
- joined_sector: int32 [2, 24576], P('node', 'sec'), may hold values from 0 to 63, as said below
- owner_map: int32 [2, 64], P('node'), may hold values from 0 to 63, each once within a row
- live_pairs: int32 [2, 64], P('node', 'sec'), may hold values from 1 to 384, as said below
Outputs:
- environment: float32 [2, 64, 128, 128], P('node', 'sec')
The draws below stay inside these ranges and needn't reach their ends.
Inputs may be any that keep to these rules, and one draw needn't show every extreme that they name: `env_blocks`: each block is symmetric. `joined_sector`: slot p belongs to tree node k = p // 3072 of its group, and its sector is one of that node's sectors k * 8 to k * 8 + 7. `owner_map`: each row names every index once. `live_pairs`: in every group some index of sec has all 384 slots live.
All inputs are finite; a program needn't handle non-finite values.
Results may differ from the reference program's by a relative error of at most 0.0003.
Values sent between devices are 32-bit elements; how exact they have to be, the bound alone decides.
A program may use at most 128 MiB of HBM per device.

```python
import math
import jax
import jax.numpy as jnp
from jax import lax

R = 128
DC = 128
SECTORS_NODE = 8
PAIRS_DEV = 384
NODES = 2
SECTORS = 64
PAIRS = 24576


def draw_env_blocks(key, part):
    base = jax.random.truncated_normal(jax.random.fold_in(key, 11), -4.0, 4.0, (NODES, PAIRS, R, R), jnp.float32)
    blocks = (base + jnp.swapaxes(base, -1, -2)) * (0.7 / math.sqrt(R)) + jnp.eye(R, dtype=jnp.float32)
    return blocks.astype(jnp.bfloat16)


def draw_iso_blocks(key, part):
    tree_count = PAIRS // (PAIRS_DEV * SECTORS_NODE)
    per_tree = PAIRS_DEV * SECTORS_NODE
    shared = jax.random.truncated_normal(jax.random.fold_in(key, 41), -4.0, 4.0, (NODES, tree_count, 1, R, DC), jnp.float32)
    logs = jax.random.uniform(jax.random.fold_in(key, 42), (NODES, tree_count, 1, 1, DC), jnp.float32, math.log(0.4), math.log(4.0))
    column_scales = jnp.exp(logs)
    own = jax.random.truncated_normal(jax.random.fold_in(key, 44), -4.0, 4.0, (NODES, tree_count, per_tree, R, DC), jnp.float32)
    mixed = 0.8 * shared + 0.6 * own
    blocks = mixed * column_scales * (1.0 / math.sqrt(R))
    return blocks.reshape(NODES, PAIRS, R, DC).astype(jnp.bfloat16)


def draw_joined_sector(key, part):
    first_draw = jax.random.randint(jax.random.fold_in(key, 31), (NODES, PAIRS), 0, SECTORS_NODE)
    second_draw = jax.random.randint(jax.random.fold_in(key, 32), (NODES, PAIRS), 0, SECTORS_NODE)
    within = jnp.minimum(first_draw, second_draw)
    slots = jnp.arange(PAIRS, dtype=jnp.int32)[None, :]
    tree_node = slots // (PAIRS_DEV * SECTORS_NODE)
    return (tree_node * SECTORS_NODE + within).astype(jnp.int32)


def draw_live_pairs(key, part):
    first_draw = jax.random.randint(jax.random.fold_in(key, 21), (NODES, SECTORS), 1, PAIRS_DEV + 1)
    second_draw = jax.random.randint(jax.random.fold_in(key, 22), (NODES, SECTORS), 1, PAIRS_DEV + 1)
    counts = jnp.minimum(first_draw, second_draw)
    chosen = jax.random.randint(jax.random.fold_in(key, 23), (NODES, 1), 0, SECTORS)
    places = jnp.arange(SECTORS, dtype=jnp.int32)[None, :]
    return jnp.where(places == chosen, PAIRS_DEV, counts).astype(jnp.int32)


def setup_inputs(seed: int = 0) -> dict:
    key_list = jax.random.split(jax.random.key(seed), 6)
    return {
        "env_blocks": draw_env_blocks(jax.random.fold_in(key_list[5], 71), 0),
        "iso_blocks": draw_iso_blocks(jax.random.fold_in(key_list[5], 71), 0),
        "joined_sector": draw_joined_sector(jax.random.fold_in(key_list[5], 71), 0),
        "owner_map": jax.vmap(lambda own: jax.random.permutation(own, SECTORS))(jax.random.split(key_list[3], NODES)).reshape((NODES, SECTORS)).astype(jnp.int32),
        "live_pairs": draw_live_pairs(jax.random.fold_in(key_list[5], 71), 0),
    }


def reference(env_blocks, iso_blocks, joined_sector, owner_map, live_pairs):
    hermitians = []
    for node_index in range(NODES):
        targets_all = owner_map[node_index][joined_sector[node_index]].astype(jnp.int32)

        def one_source(partial_value, source, node_index=node_index, targets_all=targets_all):
            first_pair = (source * PAIRS_DEV).astype(jnp.int32)
            zero_index = jnp.zeros((), jnp.int32)
            node_start = (zero_index + node_index).astype(jnp.int32)
            blocks = lax.dynamic_slice(env_blocks, (node_start, first_pair, zero_index, zero_index), (1, PAIRS_DEV, R, R))[0].astype(jnp.float32)
            weights = lax.dynamic_slice(iso_blocks, (node_start, first_pair, zero_index, zero_index), (1, PAIRS_DEV, R, DC))[0].astype(jnp.float32)
            product = jnp.einsum('prk,pkc->prc', blocks, weights, precision=lax.Precision.HIGHEST).astype(jnp.bfloat16)
            sandwich = jnp.einsum('prc,prd->pcd', weights, product.astype(jnp.float32), precision=lax.Precision.HIGHEST)
            living = jnp.arange(PAIRS_DEV, dtype=jnp.int32) < live_pairs[node_index, source]
            sandwich = jnp.where(living[:, None, None], sandwich, jnp.zeros((), jnp.float32))
            targets = lax.dynamic_slice_in_dim(targets_all, first_pair, PAIRS_DEV, 0)
            return (partial_value.at[targets].add(sandwich), None)
        zero_sums = jnp.zeros((SECTORS, DC, DC), jnp.float32)
        partial_value, unused = lax.scan(one_source, zero_sums, jnp.arange(SECTORS, dtype=jnp.int32))
        hermitian = jnp.triu(partial_value) + jnp.swapaxes(jnp.triu(partial_value, 1), 1, 2)
        hermitians.append(hermitian)
    stacked = jnp.stack(hermitians, axis=0)
    grand_total = jnp.sum(stacked * stacked)
    factor = lax.rsqrt(grand_total / (NODES * SECTORS * DC * DC) + 1e-06)
    return stacked * factor
```

```python
import functools

import jax
import jax.numpy as jnp
from jax import lax
from jax.experimental import pallas as pl
from jax.experimental.pallas import tpu as pltpu
from jax.sharding import PartitionSpec as P

MESH = pl.DeviceIdType.MESH
NODE_SECTORS = 8
CHUNK = 16
PAIRS = CHUNK // 2
DEPTH = PAIRS // 2
ROWS = 72
TOP = 40


def pack_rows(full):
    lane = lax.broadcasted_iota(jnp.int32, (16, 128), 1)
    rows = [full[112:128]]
    for low in range(3):
        high = 6 - low
        width = 16 * (high + 1)
        short = pltpu.roll(full[16 * low : 16 * low + 16], width, 1)
        rows.append(jnp.where(lane < width, full[16 * high : 16 * high + 16], short))
    rows.append(jnp.where(lane[:8] < 64, full[48:56], pltpu.roll(full[56:64], 64, 1)))
    return jnp.concatenate(rows, axis=0)


def unpack_rows(packed):
    blocks = [None] * 8
    blocks[7] = packed[0:16]
    for low in range(3):
        high = 6 - low
        width = 16 * (high + 1)
        both = packed[16 + 16 * low : 32 + 16 * low]
        blocks[high] = both
        blocks[low] = pltpu.roll(both, 128 - width, 1)
    blocks[3] = jnp.concatenate((packed[64:72], pltpu.roll(packed[64:72], 64, 1)), axis=0)
    return jnp.concatenate(blocks, axis=0)


def local_kernel(
    live_ref, sector_ref, owner_ref, env_ref, iso_ref, parts_ref, source_ref,
    env_buf, iso_buf, sums_0, sums_1, sums_2, sums_3, env_sem, iso_sem,
):
    live = live_ref[0, 0]
    chunks = (live + CHUNK - 1) // CHUNK
    sums = (sums_0, sums_1, sums_2, sums_3)

    def copies(c):
        first = pl.multiple_of(c * CHUNK, CHUNK)
        span = pl.ds(first, CHUNK)
        return (
            pltpu.make_async_copy(iso_ref.at[0, span], iso_buf.at[span], iso_sem.at[c]),
            pltpu.make_async_copy(env_ref.at[0, span], env_buf.at[span], env_sem.at[c]),
        )

    def start(c, carry):
        for copy in copies(c):
            copy.start()
        return carry

    lax.fori_loop(0, chunks, start, 0)

    def invert(sector, carry):
        source_ref[0, owner_ref[0, sector]] = sector
        return carry

    lax.fori_loop(0, owner_ref.shape[1], invert, 0)

    def clear(sector, carry):
        for ref in sums:
            ref[sector] = jnp.zeros((128, 128), jnp.float32)
        return carry

    lax.fori_loop(0, NODE_SECTORS + 1, clear, 0)

    def await_chunk(c):
        for copy in copies(c):
            copy.wait()

    def target(slot):
        return jnp.where(slot < live, lax.rem(sector_ref[0, slot], NODE_SECTORS), NODE_SECTORS)

    def stacked(c, pair):
        first = c * CHUNK + 2 * pair
        none = jnp.zeros((128, 128), jnp.bfloat16)
        top = jnp.concatenate((iso_buf[first], none), axis=1)
        bottom = jnp.concatenate((none, iso_buf[first + 1]), axis=1)
        return jnp.concatenate((top, bottom), axis=0)

    def run(z_acc, y_acc):
        def first_stage(c, pair):
            mxu, place = pair % 2, pair // 2
            first = c * CHUNK + 2 * pair
            pltpu.matmul_push_rhs(stacked(c, pair), staging_register=0, mxu_index=mxu)
            side = jnp.concatenate((env_buf[first], env_buf[first + 1]), axis=1)
            pltpu.matmul_acc_lhs(z_acc[mxu][place], side, load_staged_rhs=0)

        def turned(pair):
            mxu, place = pair % 2, pair // 2
            z = pltpu.matmul_pop(z_acc[mxu][place]).astype(jnp.bfloat16)
            return jnp.concatenate((z[:, :128].T, z[:, 128:].T), axis=1)

        def second_stage(c, pair, side):
            mxu, place = pair % 2, pair // 2
            pltpu.matmul_push_rhs(stacked(c, pair), staging_register=1, mxu_index=mxu)
            pltpu.matmul_acc_lhs(y_acc[mxu][place], side, load_staged_rhs=1)

        def add(c, pair, drop):
            mxu, place = pair % 2, pair // 2
            y = pltpu.matmul_pop(y_acc[mxu][place])
            for half in range(2):
                slot = c * CHUNK + 2 * pair + half
                where = target(jnp.maximum(slot, 0))
                where = jnp.where(drop, NODE_SECTORS, where)
                ref = sums[2 * mxu + half]
                ref[where] = ref[where] + y[:, 128 * half : 128 * half + 128]

        for pair in range(PAIRS):
            mxu, place = pair % 2, pair // 2
            pltpu.matmul_pop(z_acc[mxu][place])
            pltpu.matmul_pop(y_acc[mxu][place])
        await_chunk(0)
        for pair in range(PAIRS):
            first_stage(0, pair)

        def turn(c, carry):
            await_chunk(c)
            waiting = []
            for place in range(DEPTH):
                for mxu in range(2):
                    pair = 2 * place + mxu
                    side = turned(pair)
                    first_stage(c, pair)
                    waiting.append((pair, side))
                if place >= 1:
                    for _ in range(2):
                        pair, side = waiting.pop(0)
                        add(c - 2, pair, c < 2)
                        second_stage(c - 1, pair, side)
            while waiting:
                pair, side = waiting.pop(0)
                add(c - 2, pair, c < 2)
                second_stage(c - 1, pair, side)
            return carry

        lax.fori_loop(1, chunks, turn, 0)
        for pair in range(PAIRS):
            side = turned(pair)
            add(chunks - 2, pair, chunks < 2)
            second_stage(chunks - 1, pair, side)
        for pair in range(PAIRS):
            add(chunks - 1, pair, False)

    accs = [[pltpu.ACC(mxu)((128, 256), jnp.float32) for _ in range(DEPTH)] for mxu in range(2)]
    pl.run_scoped(run, accs, accs)

    def finish(sector, carry):
        full = (sums_0[sector] + sums_1[sector]) + (sums_2[sector] + sums_3[sector])
        parts_ref[sector] = pack_rows(full)
        return carry

    lax.fori_loop(0, NODE_SECTORS, finish, 0)


def local_sums(env_blocks, iso_blocks, joined_sector, owner_map, live_pairs):
    pairs = env_blocks.shape[1]
    smem = pl.BlockSpec(memory_space=pltpu.SMEM)
    hbm = pl.BlockSpec(memory_space=pltpu.HBM)
    return pl.pallas_call(
        local_kernel,
        out_shape=(
            jax.ShapeDtypeStruct((NODE_SECTORS, ROWS, 128), jnp.float32),
            jax.ShapeDtypeStruct(owner_map.shape, jnp.int32),
        ),
        in_specs=[smem, smem, smem, hbm, hbm],
        out_specs=(pl.BlockSpec(memory_space=pltpu.VMEM), smem),
        scratch_shapes=[
            pltpu.VMEM((pairs, 128, 128), jnp.bfloat16),
            pltpu.VMEM((pairs, 128, 128), jnp.bfloat16),
            *[pltpu.VMEM((NODE_SECTORS + 1, 128, 128), jnp.float32)] * 4,
            pltpu.SemaphoreType.DMA((pairs // CHUNK,)),
            pltpu.SemaphoreType.DMA((pairs // CHUNK,)),
        ],
        name="local_sums",
    )(live_pairs, joined_sector, owner_map, env_blocks, iso_blocks)


def exchange_kernel(
    parts_ref, source_ref, out_ref,
    got_ref, own_ref, one_top, one_low, send_top, send_low, two_top, two_low,
    square_ref, square_one, square_sum, square_two,
    sent_sem, part_sem, top_one_sem, low_one_sem, top_two_sem, low_two_sem, square_one_sem, square_two_sem,
):
    me = lax.axis_index("sec")
    node = lax.axis_index("node")
    x, y, z = me // 16, (me // 4) % 4, me % 4
    near = y + 1 - 2 * (y % 2)
    far = (y + 3 + 2 * (y % 2)) % 4
    low = ROWS - TOP

    def plane(slot):
        dy, dz = slot // 4, slot % 4
        return x, (near if dy else y), (z + dz) % 4

    def column(slot):
        dy, dx = slot // 4, slot % 4
        return (x + dx) % 4, (far if dy else y), z

    def at(place, group=None):
        return (place[0] * 16 + place[1] * 4 + place[2], node if group is None else group)

    sends = []

    def send(src, dst, sem, device):
        copy = pltpu.make_async_remote_copy(
            src_ref=src, dst_ref=dst, send_sem=sent_sem.at[len(sends)], recv_sem=sem,
            device_id=device, device_id_type=MESH,
        )
        copy.start()
        sends.append(copy)
        return copy

    barrier = pltpu.get_barrier_semaphore()
    for slot in range(1, 8):
        pl.semaphore_signal(barrier, inc=1, device_id=at(plane(slot)), device_id_type=MESH)
        pl.semaphore_signal(barrier, inc=1, device_id=at(column(slot)), device_id_type=MESH)
    for slot in range(8):
        pl.semaphore_signal(barrier, inc=1, device_id=at(column(slot), 1 - node), device_id_type=MESH)
    pl.semaphore_wait(barrier, 22)

    part_copies = []
    for slot in range(1, 8):
        place = plane(slot)
        member = (place[1] % 2) * 4 + place[2]
        part_copies.append(
            send(parts_ref.at[member], got_ref.at[slot - 1], part_sem.at[slot - 1], at(place))
        )

    def cut(source):
        return source // 16, (source // 4) % 4, source % 4

    top_pick, low_pick = [], []
    for slot in range(8):
        xs, ys, zs = cut(source_ref[0, at(plane(slot))[0]])
        top_pick.append(jnp.where(ys == y, 0, 4) + (x + 4 - xs) % 4)
        xs, ys, zs = cut(source_ref[0, at(column(slot))[0]])
        low_pick.append(jnp.where(ys == y, 0, 4) + (z + 4 - zs) % 4)
    xs, ys, zs = cut(source_ref[0, me])
    far_s = (ys + 3 + 2 * (ys % 2)) % 4
    same = (y // 2) == (ys // 2)
    middle = jnp.where(same, ys, far_s)
    top_take = jnp.where(middle == y, 0, 4) + (z + 4 - zs) % 4
    low_take = jnp.where(same, 0, 4) + (x + 4 - xs) % 4

    row = lax.broadcasted_iota(jnp.int32, (128, 128), 0)
    lane = lax.broadcasted_iota(jnp.int32, (128, 128), 1)

    total = parts_ref[(y % 2) * 4 + z]
    for slot in range(1, 8):
        part_copies[slot - 1].wait_recv()
        total = total + got_ref[slot - 1]
    own_ref[...] = total
    one_top[0] = total[:TOP]
    one_low[0] = total[TOP:]

    top_copies, low_copies = [], []
    for slot in range(1, 8):
        top_copies.append(
            send(own_ref.at[pl.ds(0, TOP)], one_top.at[slot], top_one_sem.at[slot - 1], at(column(slot)))
        )
        low_copies.append(
            send(own_ref.at[pl.ds(TOP, low)], one_low.at[slot], low_one_sem.at[slot - 1], at(plane(slot)))
        )

    full = unpack_rows(total)
    weighed = jnp.where(row > lane, 2.0 * (full * full), jnp.where(row == lane, full * full, 0.0))
    squares = jnp.sum(weighed.reshape(16, 8, 128), axis=0)
    square_ref[...] = squares
    square_copies = []
    for index in range(1, 16):
        group = node if index < 8 else 1 - node
        square_copies.append(
            send(square_ref, square_one.at[index - 1], square_one_sem.at[index - 1], at(column(index % 8), group))
        )
    for index in range(1, 16):
        square_copies[index - 1].wait_recv()
        squares = squares + square_one[index - 1]
    square_sum[...] = squares
    square_copies = []
    for slot in range(1, 8):
        square_copies.append(
            send(square_sum, square_two.at[slot - 1], square_two_sem.at[slot - 1], at(plane(slot)))
        )

    for copy in top_copies:
        copy.wait_recv()
    for slot in range(1, 8):
        send_top[slot - 1] = one_top[top_pick[slot]]
    two_top[0] = one_top[top_pick[0]]
    top_copies = []
    for slot in range(1, 8):
        top_copies.append(
            send(send_top.at[slot - 1], two_top.at[slot], top_two_sem.at[slot - 1], at(plane(slot)))
        )
    for copy in low_copies:
        copy.wait_recv()
    for slot in range(1, 8):
        send_low[slot - 1] = one_low[low_pick[slot]]
    two_low[0] = one_low[low_pick[0]]
    low_copies = []
    for slot in range(1, 8):
        low_copies.append(
            send(send_low.at[slot - 1], two_low.at[slot], low_two_sem.at[slot - 1], at(column(slot)))
        )

    for slot in range(1, 8):
        square_copies[slot - 1].wait_recv()
        squares = squares + square_two[slot - 1]
    entries = 2 * 64 * 128 * 128
    factor = lax.rsqrt(jnp.sum(squares, keepdims=True) / entries + 1e-06)

    for copy in top_copies + low_copies:
        copy.wait_recv()
    full = unpack_rows(jnp.concatenate((two_top[top_take], two_low[low_take]), axis=0)) * factor
    lower = jnp.where(row >= lane, full, 0.0)
    out_ref[0, 0] = jnp.where(row >= lane, full, lower.T)

    for copy in sends:
        copy.wait_send()


def exchange(parts, source):
    low = ROWS - TOP
    f32 = jnp.float32
    dma = pltpu.SemaphoreType.DMA
    return pl.pallas_call(
        exchange_kernel,
        out_shape=jax.ShapeDtypeStruct((1, 1, 128, 128), f32),
        in_specs=[pl.BlockSpec(memory_space=pltpu.VMEM), pl.BlockSpec(memory_space=pltpu.SMEM)],
        out_specs=pl.BlockSpec(memory_space=pltpu.VMEM),
        scratch_shapes=[
            pltpu.VMEM((7, ROWS, 128), f32),
            pltpu.VMEM((ROWS, 128), f32),
            pltpu.VMEM((8, TOP, 128), f32),
            pltpu.VMEM((8, low, 128), f32),
            pltpu.VMEM((7, TOP, 128), f32),
            pltpu.VMEM((7, low, 128), f32),
            pltpu.VMEM((8, TOP, 128), f32),
            pltpu.VMEM((8, low, 128), f32),
            pltpu.VMEM((8, 128), f32),
            pltpu.VMEM((15, 8, 128), f32),
            pltpu.VMEM((8, 128), f32),
            pltpu.VMEM((7, 8, 128), f32),
            dma((57,)),
            dma((7,)), dma((7,)), dma((7,)), dma((7,)), dma((7,)), dma((15,)), dma((7,)),
        ],
        compiler_params=pltpu.CompilerParams(collective_id=0, has_side_effects=True),
        name="exchange",
    )(parts, source)


def body(env_blocks, iso_blocks, joined_sector, owner_map, live_pairs):
    parts, source = local_sums(env_blocks, iso_blocks, joined_sector, owner_map, live_pairs)
    return exchange(parts, source)


def solution(mesh):
    placed = (
        P("node", "sec", None, None),
        P("node", "sec", None, None),
        P("node", "sec"),
        P("node", None),
        P("node", "sec"),
    )
    return jax.shard_map(
        body, mesh=mesh, in_specs=placed, out_specs=P("node", "sec", None, None), check_vma=False
    )
```

```python
import functools

import jax
import jax.numpy as jnp
from jax import lax
from jax.experimental import pallas as pl
from jax.experimental.pallas import tpu as pltpu
from jax.sharding import PartitionSpec as P

MESH = pl.DeviceIdType.MESH
NODE_SECTORS = 8
CHUNK = 16
PAIRS = CHUNK // 2
DEPTH = PAIRS // 2
ROWS = 72
TOP = 40


def pack_rows(full):
    lane = lax.broadcasted_iota(jnp.int32, (16, 128), 1)
    rows = [full[112:128]]
    for low in range(3):
        high = 6 - low
        width = 16 * (high + 1)
        short = pltpu.roll(full[16 * low : 16 * low + 16], width, 1)
        rows.append(jnp.where(lane < width, full[16 * high : 16 * high + 16], short))
    rows.append(jnp.where(lane[:8] < 64, full[48:56], pltpu.roll(full[56:64], 64, 1)))
    return jnp.concatenate(rows, axis=0)


def unpack_rows(packed):
    blocks = [None] * 8
    blocks[7] = packed[0:16]
    for low in range(3):
        high = 6 - low
        width = 16 * (high + 1)
        both = packed[16 + 16 * low : 32 + 16 * low]
        blocks[high] = both
        blocks[low] = pltpu.roll(both, 128 - width, 1)
    blocks[3] = jnp.concatenate((packed[64:72], pltpu.roll(packed[64:72], 64, 1)), axis=0)
    return jnp.concatenate(blocks, axis=0)


def local_kernel(
    live_ref, sector_hbm, owner_hbm, env_ref, iso_ref, parts_ref, source_ref,
    sector_ref, owner_ref, env_buf, iso_buf, carry_buf,
    sums_0, sums_1, sums_2, sums_3, env_sem, iso_sem, small_sem,
):
    slots = env_buf.shape[0]
    sums = (sums_0, sums_1, sums_2, sums_3)

    def copies(c):
        first = pl.multiple_of(c * CHUNK, CHUNK)
        span = pl.ds(first, CHUNK)
        return (
            pltpu.make_async_copy(iso_ref.at[0, span], iso_buf.at[span], iso_sem.at[c]),
            pltpu.make_async_copy(env_ref.at[0, span], env_buf.at[span], env_sem.at[c]),
        )

    def start(c, carry):
        for copy in copies(c):
            copy.start()
        return carry

    small = [
        pltpu.make_async_copy(src, dst, small_sem.at[i])
        for i, (src, dst) in enumerate(
            ((sector_hbm, sector_ref), (owner_hbm, owner_ref))
        )
    ]
    for copy in small:
        copy.start()
    lax.fori_loop(0, slots // CHUNK, start, 0)

    def clear(sector, carry):
        for ref in sums:
            ref[sector] = jnp.zeros((128, 128), jnp.float32)
        return carry

    lax.fori_loop(0, NODE_SECTORS + 1, clear, 0)
    for copy in small:
        copy.wait()
    live = live_ref[0, 0]
    doubles = (live + 2 * CHUNK - 1) // (2 * CHUNK)
    last = 2 * doubles - 1

    def invert(sector, carry):
        source_ref[0, owner_ref[0, sector]] = sector
        return carry

    lax.fori_loop(0, owner_ref.shape[1], invert, 0, unroll=8)

    def await_chunk(c):
        for copy in copies(c):
            copy.wait()

    def target(slot):
        counts = jnp.logical_and(slot >= 0, slot < live)
        return jnp.where(counts, lax.rem(sector_ref[0, jnp.maximum(slot, 0)], NODE_SECTORS), NODE_SECTORS)

    def stage(c, place, mxu, register):
        first = c * CHUNK + 2 * (2 * place + mxu)
        none = jnp.zeros((128, 128), jnp.bfloat16)
        top = jnp.concatenate((iso_buf[first], none), axis=1)
        bottom = jnp.concatenate((none, iso_buf[first + 1]), axis=1)
        pltpu.matmul_push_rhs(
            jnp.concatenate((top, bottom), axis=0), staging_register=register, mxu_index=mxu
        )

    def run(z_acc, y_acc):
        def turned(place, mxu):
            z = pltpu.matmul_pop(z_acc[mxu][place]).astype(jnp.bfloat16)
            return jnp.concatenate((z[:, :128].T, z[:, 128:].T), axis=1)

        def first_stage(c, place, mxu, register):
            stage(c, place, mxu, register)
            first = c * CHUNK + 2 * (2 * place + mxu)
            side = jnp.concatenate((env_buf[first], env_buf[first + 1]), axis=1)
            pltpu.matmul_acc_lhs(z_acc[mxu][place], side, load_staged_rhs=register)

        def add(c, place, mxu):
            y = pltpu.matmul_pop(y_acc[mxu][place])
            for half in range(2):
                where = target(c * CHUNK + 2 * (2 * place + mxu) + half)
                ref = sums[2 * mxu + half]
                ref[where] = ref[where] + y[:, 128 * half : 128 * half + 128]

        def second_stage(place, mxu, register, side):
            pltpu.matmul_acc_lhs(y_acc[mxu][place], side, load_staged_rhs=register)

        both = range(2)

        def turn(c, sides):
            for mxu in both:
                add(c - 3, 3, mxu)
                second_stage(3, mxu, 0, sides[mxu])
            turns = []
            for place in range(2):
                turns.append([turned(place, mxu) for mxu in both])
                for mxu in both:
                    first_stage(c, place, mxu, 1 - place)
            for mxu in both:
                add(c - 2, 0, mxu)
                stage(c - 1, 0, mxu, 1)
                second_stage(0, mxu, 1, turns[0][mxu])
            for place in range(2, 4):
                turns.append([turned(place, mxu) for mxu in both])
                for mxu in both:
                    first_stage(c, place, mxu, 0)
                for mxu in both:
                    add(c - 2, place - 1, mxu)
                    stage(c - 1, place - 1, mxu, 1)
                    second_stage(place - 1, mxu, 1, turns[place - 1][mxu])
            for mxu in both:
                stage(c - 1, 3, mxu, 0)
            return turns[3]

        for place in range(DEPTH):
            for mxu in both:
                pltpu.matmul_pop(z_acc[mxu][place])
                pltpu.matmul_pop(y_acc[mxu][place])
        await_chunk(0)
        for place in range(DEPTH):
            for mxu in both:
                first_stage(0, place, mxu, place % 2)
        for mxu in both:
            stage(0, 3, mxu, 0)
            carry_buf[mxu] = jnp.zeros((128, 256), jnp.bfloat16)

        def double(step, carry):
            c = 2 * step + 1
            await_chunk(c)
            await_chunk(c + 1)
            sides = turn(c, [carry_buf[mxu] for mxu in both])
            sides = turn(c + 1, sides)
            for mxu in both:
                carry_buf[mxu] = sides[mxu]
            return carry

        lax.fori_loop(0, doubles - 1, double, 0)
        await_chunk(last)
        sides = turn(last, [carry_buf[mxu] for mxu in both])
        turns = [[turned(place, mxu) for mxu in both] for place in range(2)]
        for mxu in both:
            add(last - 2, 3, mxu)
            second_stage(3, mxu, 0, sides[mxu])
        for place in range(2, 4):
            turns.append([turned(place, mxu) for mxu in both])
        for place in range(4):
            for mxu in both:
                add(last - 1, place, mxu)
                stage(last, place, mxu, 1 - place % 2)
                second_stage(place, mxu, 1 - place % 2, turns[place][mxu])
        for place in range(4):
            for mxu in both:
                add(last, place, mxu)

    accs = [[pltpu.ACC(mxu)((128, 256), jnp.float32) for _ in range(DEPTH)] for mxu in range(2)]
    pl.run_scoped(run, accs, accs)

    for sector in range(NODE_SECTORS):
        full = (sums_0[sector] + sums_1[sector]) + (sums_2[sector] + sums_3[sector])
        parts_ref[sector] = pack_rows(full)

    def rest(c, carry):
        await_chunk(c)
        return carry

    lax.fori_loop(last + 1, slots // CHUNK, rest, 0)


def local_sums(env_blocks, iso_blocks, joined_sector, owner_map, live_pairs):
    pairs = env_blocks.shape[1]
    hbm = pl.BlockSpec(memory_space=pltpu.HBM)
    return pl.pallas_call(
        local_kernel,
        out_shape=(
            pltpu.VMEM((NODE_SECTORS, ROWS, 128), jnp.float32),
            pltpu.SMEM(owner_map.shape, jnp.int32),
        ),
        in_specs=[pl.BlockSpec(memory_space=pltpu.SMEM)] + [hbm] * 4,
        out_specs=(pl.BlockSpec(memory_space=pltpu.VMEM), pl.BlockSpec(memory_space=pltpu.SMEM)),
        scratch_shapes=[
            pltpu.SMEM(joined_sector.shape, jnp.int32),
            pltpu.SMEM(owner_map.shape, jnp.int32),
            pltpu.VMEM((pairs, 128, 128), jnp.bfloat16),
            pltpu.VMEM((pairs, 128, 128), jnp.bfloat16),
            pltpu.VMEM((2, 128, 256), jnp.bfloat16),
            *[pltpu.VMEM((NODE_SECTORS + 1, 128, 128), jnp.float32)] * 4,
            pltpu.SemaphoreType.DMA((pairs // CHUNK,)),
            pltpu.SemaphoreType.DMA((pairs // CHUNK,)),
            pltpu.SemaphoreType.DMA((2,)),
        ],
        compiler_params=pltpu.CompilerParams(vmem_limit_bytes=40 * 2**20),
        name="local_sums",
    )(live_pairs, *[
        pltpu.with_memory_space_constraint(array, pltpu.HBM)
        for array in (joined_sector, owner_map, env_blocks, iso_blocks)
    ])


def exchange_kernel(
    parts_ref, source_ref, rows_ref, squares_ref,
    got_ref, own_ref, one_top, one_low, send_top, send_low, two_top, two_low,
    square_own, square_one, square_group, square_side, square_both, square_two, sent_sem, got_sem,
):
    me = lax.axis_index("sec")
    node = lax.axis_index("node")
    x, y, z = me // 16, (me // 4) % 4, me % 4
    near = y + 1 - 2 * (y % 2)
    far = (y + 3 + 2 * (y % 2)) % 4
    low = ROWS - TOP
    order = (6, 2, 5, 7, 1, 3, 4)

    def plane(slot):
        dy, dz = slot // 4, slot % 4
        return x * 16 + (near if dy else y) * 4 + (z + dz) % 4

    def column(slot):
        dy, dx = slot // 4, slot % 4
        return (x + dx) % 4 * 16 + (far if dy else y) * 4 + z

    def send(src, dst, phase, place, group=node):
        pltpu.make_async_remote_copy(
            src_ref=src, dst_ref=dst, send_sem=sent_sem.at[phase], recv_sem=got_sem.at[phase],
            device_id=(place, group), device_id_type=MESH,
        ).start()

    def landed(ref, phase):
        pltpu.make_async_copy(ref, ref, got_sem.at[phase]).wait()

    def left(ref, phase):
        pltpu.make_async_copy(ref, ref, sent_sem.at[phase]).wait()

    barrier = pltpu.get_barrier_semaphore()
    for slot in order:
        pl.semaphore_signal(barrier, inc=1, device_id=(plane(slot), node), device_id_type=MESH)
    for slot in order:
        pl.semaphore_signal(barrier, inc=1, device_id=(column(slot), node), device_id_type=MESH)
    pl.semaphore_signal(barrier, inc=1, device_id=(me, 1 - node), device_id_type=MESH)
    pl.semaphore_wait(barrier, 15)

    for slot in order:
        member = plane(slot) % 8
        send(parts_ref.at[member], got_ref.at[slot - 1], 0, plane(slot))

    def cut(source):
        return source // 16, (source // 4) % 4, source % 4

    top_pick, low_pick = [], []
    for slot in range(8):
        xs, ys, zs = cut(source_ref[0, plane(slot)])
        top_pick.append(jnp.where(ys == y, 0, 4) + (x + 4 - xs) % 4)
        xs, ys, zs = cut(source_ref[0, column(slot)])
        low_pick.append(jnp.where(ys == y, 0, 4) + (z + 4 - zs) % 4)
    xs, ys, zs = cut(source_ref[0, me])
    far_s = (ys + 3 + 2 * (ys % 2)) % 4
    same = (y // 2) == (ys // 2)
    middle = jnp.where(same, ys, far_s)
    top_take = jnp.where(middle == y, 0, 4) + (z + 4 - zs) % 4
    low_take = jnp.where(same, 0, 4) + (x + 4 - xs) % 4

    row = lax.broadcasted_iota(jnp.int32, (128, 128), 0)
    lane = lax.broadcasted_iota(jnp.int32, (128, 128), 1)

    total = parts_ref[me % 8]
    landed(got_ref, 0)
    for slot in range(7):
        total = total + got_ref[slot]
    own_ref[...] = total
    one_top[0] = total[:TOP]
    one_low[0] = total[TOP:]

    for slot in order:
        send(own_ref.at[pl.ds(TOP, low)], one_low.at[slot], 1, plane(slot))
    full = unpack_rows(total)
    squared = full * full
    weighed = jnp.where(row > lane, squared + squared, jnp.where(row == lane, squared, 0.0))
    squares = jnp.sum(weighed.reshape(16, 8, 128), axis=0)
    square_own[...] = squares
    for slot in order:
        send(square_own, square_one.at[slot - 1], 2, column(slot))
    for slot in order:
        send(own_ref.at[pl.ds(0, TOP)], one_top.at[slot], 3, column(slot))
    landed(square_one, 2)
    for slot in range(7):
        squares = squares + square_one[slot]
    square_group[...] = squares
    send(square_group, square_side, 4, me, 1 - node)

    landed(one_low.at[pl.ds(1, 7)], 1)
    for slot in range(1, 8):
        send_low[slot - 1] = one_low[low_pick[slot]]
    two_low[0] = one_low[low_pick[0]]
    for slot in order:
        send(send_low.at[slot - 1], two_low.at[slot], 5, column(slot))
    landed(square_side, 4)
    squares = squares + square_side[...]
    square_both[...] = squares
    for slot in order:
        send(square_both, square_two.at[slot - 1], 6, plane(slot))
    landed(one_top.at[pl.ds(1, 7)], 3)
    for slot in range(1, 8):
        send_top[slot - 1] = one_top[top_pick[slot]]
    two_top[0] = one_top[top_pick[0]]
    for slot in order:
        send(send_top.at[slot - 1], two_top.at[slot], 7, plane(slot))

    landed(square_two, 6)
    for slot in range(7):
        squares = squares + square_two[slot]
    squares_ref[...] = squares
    left(got_ref, 0)
    left(send_low, 1)
    left(square_one, 2)
    left(send_top, 3)
    left(square_side, 4)
    left(square_two, 6)
    landed(two_low.at[pl.ds(1, 7)], 5)
    rows_ref[pl.ds(TOP, low)] = two_low[low_take]
    landed(two_top.at[pl.ds(1, 7)], 7)
    rows_ref[pl.ds(0, TOP)] = two_top[top_take]
    left(send_low, 5)
    left(send_top, 7)


def exchange(parts, source):
    low = ROWS - TOP
    f32 = jnp.float32
    vmem = pl.BlockSpec(memory_space=pltpu.VMEM)
    return pl.pallas_call(
        exchange_kernel,
        out_shape=(pltpu.VMEM((ROWS, 128), f32), pltpu.VMEM((8, 128), f32)),
        in_specs=[vmem, pl.BlockSpec(memory_space=pltpu.SMEM)],
        out_specs=(vmem, vmem),
        scratch_shapes=[
            pltpu.VMEM((7, ROWS, 128), f32),
            pltpu.VMEM((ROWS, 128), f32),
            pltpu.VMEM((8, TOP, 128), f32),
            pltpu.VMEM((8, low, 128), f32),
            pltpu.VMEM((7, TOP, 128), f32),
            pltpu.VMEM((7, low, 128), f32),
            pltpu.VMEM((8, TOP, 128), f32),
            pltpu.VMEM((8, low, 128), f32),
            pltpu.VMEM((8, 128), f32),
            pltpu.VMEM((7, 8, 128), f32),
            pltpu.VMEM((8, 128), f32),
            pltpu.VMEM((8, 128), f32),
            pltpu.VMEM((8, 128), f32),
            pltpu.VMEM((7, 8, 128), f32),
            pltpu.SemaphoreType.DMA((8,)),
            pltpu.SemaphoreType.DMA((8,)),
        ],
        compiler_params=pltpu.CompilerParams(
            collective_id=0, has_side_effects=True, vmem_limit_bytes=8 * 2**20
        ),
        name="exchange",
    )(
        pltpu.with_memory_space_constraint(parts, pltpu.VMEM),
        pltpu.with_memory_space_constraint(source, pltpu.SMEM),
    )


def finish_kernel(rows_ref, squares_ref, out_ref):
    row = lax.broadcasted_iota(jnp.int32, (128, 128), 0)
    lane = lax.broadcasted_iota(jnp.int32, (128, 128), 1)
    entries = 2 * 64 * 128 * 128
    factor = lax.rsqrt(jnp.sum(squares_ref[...], keepdims=True) / entries + 1e-06)
    full = unpack_rows(rows_ref[...])
    lower = jnp.where(row >= lane, full, 0.0)
    out_ref[0, 0] = jnp.where(row >= lane, full, lower.T) * factor


def finish(rows, squares):
    vmem = pl.BlockSpec(memory_space=pltpu.VMEM)
    return pl.pallas_call(
        finish_kernel,
        out_shape=jax.ShapeDtypeStruct((1, 1, 128, 128), jnp.float32),
        in_specs=[vmem, vmem],
        out_specs=vmem,
        compiler_params=pltpu.CompilerParams(vmem_limit_bytes=8 * 2**20),
        name="finish",
    )(
        pltpu.with_memory_space_constraint(rows, pltpu.VMEM),
        pltpu.with_memory_space_constraint(squares, pltpu.VMEM),
    )


def body(env_blocks, iso_blocks, joined_sector, owner_map, live_pairs):
    parts, source = local_sums(env_blocks, iso_blocks, joined_sector, owner_map, live_pairs)
    return finish(*exchange(parts, source))


def solution(mesh):
    placed = (
        P("node", "sec", None, None),
        P("node", "sec", None, None),
        P("node", "sec"),
        P("node", None),
        P("node", "sec"),
    )
    return jax.shard_map(
        body, mesh=mesh, in_specs=placed, out_specs=P("node", "sec", None, None), check_vma=False
    )
```

```python
import functools

import jax
import jax.numpy as jnp
from jax import lax
from jax.experimental import pallas as pl
from jax.experimental.pallas import tpu as pltpu
from jax.sharding import PartitionSpec as P

MESH = pl.DeviceIdType.MESH
NODE_SECTORS = 8
CHUNK = 16
PAIRS = CHUNK // 2
DEPTH = PAIRS // 2
ROWS = 72
TOP = 40


def pack_rows(full):
    lane = lax.broadcasted_iota(jnp.int32, (16, 128), 1)
    rows = [full[112:128]]
    for low in range(3):
        high = 6 - low
        width = 16 * (high + 1)
        short = pltpu.roll(full[16 * low : 16 * low + 16], width, 1)
        rows.append(jnp.where(lane < width, full[16 * high : 16 * high + 16], short))
    rows.append(jnp.where(lane[:8] < 64, full[48:56], pltpu.roll(full[56:64], 64, 1)))
    return jnp.concatenate(rows, axis=0)


def unpack_rows(packed):
    blocks = [None] * 8
    blocks[7] = packed[0:16]
    for low in range(3):
        high = 6 - low
        width = 16 * (high + 1)
        both = packed[16 + 16 * low : 32 + 16 * low]
        blocks[high] = both
        blocks[low] = pltpu.roll(both, 128 - width, 1)
    blocks[3] = jnp.concatenate((packed[64:72], pltpu.roll(packed[64:72], 64, 1)), axis=0)
    return jnp.concatenate(blocks, axis=0)


def local_kernel(
    live_ref, sector_hbm, owner_hbm, env_ref, iso_ref, parts_ref, source_ref,
    sector_ref, owner_ref, env_buf, iso_buf, carry_buf,
    sums_0, sums_1, sums_2, sums_3, load_sem, small_sem,
):
    live = live_ref[0, 0]
    turns = 2
    loops = (live + turns * CHUNK - 1) // (turns * CHUNK)
    last = turns * loops - 1
    sums = (sums_0, sums_1, sums_2, sums_3)

    def begin(first, length, sem):
        span = pl.ds(first, length)
        pltpu.make_async_copy(iso_ref.at[0, span], iso_buf.at[span], load_sem.at[sem]).start()
        pltpu.make_async_copy(env_ref.at[0, span], env_buf.at[span], load_sem.at[sem]).start()

    def arrived(length, sem):
        both = iso_buf.at[pl.ds(0, 2 * length)]
        pltpu.make_async_copy(both, both, load_sem.at[sem]).wait()

    def begin_two(i, carry):
        begin(pl.multiple_of((2 * i - 1) * CHUNK, CHUNK), 2 * CHUNK, i)
        return carry

    small = [
        pltpu.make_async_copy(src, dst, small_sem.at[i])
        for i, (src, dst) in enumerate(
            ((sector_hbm, sector_ref), (owner_hbm, owner_ref))
        )
    ]
    for copy in small:
        copy.start()
    begin(0, CHUNK, 0)
    lax.fori_loop(1, (last + 1) // 2, begin_two, 0)
    begin(pl.multiple_of(last * CHUNK, CHUNK), CHUNK, (last + 1) // 2)

    def clear(sector, carry):
        for ref in sums:
            ref[sector] = jnp.zeros((128, 128), jnp.float32)
        return carry

    lax.fori_loop(0, NODE_SECTORS + 1, clear, 0)
    for copy in small:
        copy.wait()
    def invert(sector, carry):
        source_ref[0, owner_ref[0, sector]] = sector
        return carry

    lax.fori_loop(0, owner_ref.shape[1], invert, 0, unroll=8)

    def target(slot):
        counts = jnp.logical_and(slot >= 0, slot < live)
        return jnp.where(counts, lax.rem(sector_ref[0, jnp.maximum(slot, 0)], NODE_SECTORS), NODE_SECTORS)

    def stage(c, place, mxu, register):
        first = c * CHUNK + 2 * (2 * place + mxu)
        none = jnp.zeros((128, 128), jnp.bfloat16)
        top = jnp.concatenate((iso_buf[first], none), axis=1)
        bottom = jnp.concatenate((none, iso_buf[first + 1]), axis=1)
        pltpu.matmul_push_rhs(
            jnp.concatenate((top, bottom), axis=0), staging_register=register, mxu_index=mxu
        )

    def run(z_acc, y_acc):
        def turned(place, mxu):
            z = pltpu.matmul_pop(z_acc[mxu][place]).astype(jnp.bfloat16)
            return jnp.concatenate((z[:, :128].T, z[:, 128:].T), axis=1)

        def first_stage(c, place, mxu, register):
            stage(c, place, mxu, register)
            first = c * CHUNK + 2 * (2 * place + mxu)
            side = jnp.concatenate((env_buf[first], env_buf[first + 1]), axis=1)
            pltpu.matmul_acc_lhs(z_acc[mxu][place], side, load_staged_rhs=register)

        def add(c, place, mxu):
            y = pltpu.matmul_pop(y_acc[mxu][place])
            for half in range(2):
                where = target(c * CHUNK + 2 * (2 * place + mxu) + half)
                ref = sums[2 * mxu + half]
                ref[where] = ref[where] + y[:, 128 * half : 128 * half + 128]

        def second_stage(place, mxu, register, side):
            pltpu.matmul_acc_lhs(y_acc[mxu][place], side, load_staged_rhs=register)

        both = range(2)

        def turn(c, sides):
            for mxu in both:
                add(c - 3, 3, mxu)
                second_stage(3, mxu, 0, sides[mxu])
            ready = []
            for place in range(2):
                ready.append([turned(place, mxu) for mxu in both])
                for mxu in both:
                    first_stage(c, place, mxu, 1 - place)
            for mxu in both:
                add(c - 2, 0, mxu)
                stage(c - 1, 0, mxu, 1)
                second_stage(0, mxu, 1, ready[0][mxu])
            for place in range(2, 4):
                ready.append([turned(place, mxu) for mxu in both])
                for mxu in both:
                    first_stage(c, place, mxu, 0)
                for mxu in both:
                    add(c - 2, place - 1, mxu)
                    stage(c - 1, place - 1, mxu, 1)
                    second_stage(place - 1, mxu, 1, ready[place - 1][mxu])
            for mxu in both:
                stage(c - 1, 3, mxu, 0)
            return ready[3]

        for place in range(DEPTH):
            for mxu in both:
                pltpu.matmul_pop(z_acc[mxu][place])
                pltpu.matmul_pop(y_acc[mxu][place])
        arrived(CHUNK, 0)
        for place in range(DEPTH):
            for mxu in both:
                first_stage(0, place, mxu, place % 2)
        for mxu in both:
            stage(0, 3, mxu, 0)
            carry_buf[mxu] = jnp.zeros((128, 256), jnp.bfloat16)

        def many(step, carry):
            c = turns * step + 1
            arrived(2 * CHUNK, turns // 2 * step + 1)
            sides = [carry_buf[mxu] for mxu in both]
            sides = turn(c, sides)
            sides = turn(c + 1, sides)
            for mxu in both:
                carry_buf[mxu] = sides[mxu]
            return carry

        lax.fori_loop(0, loops - 1, many, 0)
        sides = [carry_buf[mxu] for mxu in both]
        arrived(CHUNK, (last + 1) // 2)
        sides = turn(last, sides)
        drained = [[turned(place, mxu) for mxu in both] for place in range(2)]
        for mxu in both:
            add(last - 2, 3, mxu)
            second_stage(3, mxu, 0, sides[mxu])
        for place in range(2, 4):
            drained.append([turned(place, mxu) for mxu in both])
        for place in range(4):
            for mxu in both:
                add(last - 1, place, mxu)
                stage(last, place, mxu, 1 - place % 2)
                second_stage(place, mxu, 1 - place % 2, drained[place][mxu])
        for place in range(4):
            for mxu in both:
                add(last, place, mxu)

    accs = [[pltpu.ACC(mxu)((128, 256), jnp.float32) for _ in range(DEPTH)] for mxu in range(2)]
    pl.run_scoped(run, accs, accs)

    for sector in range(NODE_SECTORS):
        full = (sums_0[sector] + sums_1[sector]) + (sums_2[sector] + sums_3[sector])
        parts_ref[sector] = pack_rows(full)


def local_sums(env_blocks, iso_blocks, joined_sector, owner_map, live_pairs):
    pairs = env_blocks.shape[1]
    hbm = pl.BlockSpec(memory_space=pltpu.HBM)
    return pl.pallas_call(
        local_kernel,
        out_shape=(
            pltpu.VMEM((NODE_SECTORS, ROWS, 128), jnp.float32),
            pltpu.SMEM(owner_map.shape, jnp.int32),
        ),
        in_specs=[pl.BlockSpec(memory_space=pltpu.SMEM)] + [hbm] * 4,
        out_specs=(pl.BlockSpec(memory_space=pltpu.VMEM), pl.BlockSpec(memory_space=pltpu.SMEM)),
        scratch_shapes=[
            pltpu.SMEM(joined_sector.shape, jnp.int32),
            pltpu.SMEM(owner_map.shape, jnp.int32),
            pltpu.VMEM((pairs, 128, 128), jnp.bfloat16),
            pltpu.VMEM((pairs, 128, 128), jnp.bfloat16),
            pltpu.VMEM((2, 128, 256), jnp.bfloat16),
            *[pltpu.VMEM((NODE_SECTORS + 1, 128, 128), jnp.float32)] * 4,
            pltpu.SemaphoreType.DMA((pairs // (2 * CHUNK) + 1,)),
            pltpu.SemaphoreType.DMA((2,)),
        ],
        compiler_params=pltpu.CompilerParams(
            vmem_limit_bytes=40 * 2**20,
        ),
        name="local_sums",
    )(live_pairs, *[
        pltpu.with_memory_space_constraint(array, pltpu.HBM)
        for array in (joined_sector, owner_map, env_blocks, iso_blocks)
    ])


def exchange_kernel(
    parts_ref, source_ref, rows_ref, squares_ref,
    got_ref, own_ref, one_top, one_low, send_top, send_low, two_top, two_low,
    square_own, square_one, square_group, square_side, square_both, square_two, sent_sem, got_sem,
):
    me = lax.axis_index("sec")
    node = lax.axis_index("node")
    x, y, z = me // 16, (me // 4) % 4, me % 4
    near = y + 1 - 2 * (y % 2)
    far = (y + 3 + 2 * (y % 2)) % 4
    low = ROWS - TOP
    order = (6, 2, 5, 7, 1, 3, 4)

    def plane(slot):
        dy, dz = slot // 4, slot % 4
        return x * 16 + (near if dy else y) * 4 + (z + dz) % 4

    def column(slot):
        dy, dx = slot // 4, slot % 4
        return (x + dx) % 4 * 16 + (far if dy else y) * 4 + z

    def send(src, dst, phase, place, group=node):
        pltpu.make_async_remote_copy(
            src_ref=src, dst_ref=dst, send_sem=sent_sem.at[phase], recv_sem=got_sem.at[phase],
            device_id=(place, group), device_id_type=MESH,
        ).start()

    def landed(ref, phase):
        pltpu.make_async_copy(ref, ref, got_sem.at[phase]).wait()

    def left(ref, phase):
        pltpu.make_async_copy(ref, ref, sent_sem.at[phase]).wait()

    barrier = pltpu.get_barrier_semaphore()
    for slot in order:
        pl.semaphore_signal(barrier, inc=1, device_id=(plane(slot), node), device_id_type=MESH)
    for slot in order:
        pl.semaphore_signal(barrier, inc=1, device_id=(column(slot), node), device_id_type=MESH)
    pl.semaphore_signal(barrier, inc=1, device_id=(me, 1 - node), device_id_type=MESH)
    pl.semaphore_wait(barrier, 15)

    for slot in order:
        member = plane(slot) % 8
        send(parts_ref.at[member], got_ref.at[slot - 1], 0, plane(slot))

    def cut(source):
        return source // 16, (source // 4) % 4, source % 4

    top_pick, low_pick = [], []
    for slot in range(8):
        xs, ys, zs = cut(source_ref[0, plane(slot)])
        top_pick.append(jnp.where(ys == y, 0, 4) + (x + 4 - xs) % 4)
        xs, ys, zs = cut(source_ref[0, column(slot)])
        low_pick.append(jnp.where(ys == y, 0, 4) + (z + 4 - zs) % 4)
    xs, ys, zs = cut(source_ref[0, me])
    far_s = (ys + 3 + 2 * (ys % 2)) % 4
    same = (y // 2) == (ys // 2)
    middle = jnp.where(same, ys, far_s)
    top_take = jnp.where(middle == y, 0, 4) + (z + 4 - zs) % 4
    low_take = jnp.where(same, 0, 4) + (x + 4 - xs) % 4

    row = lax.broadcasted_iota(jnp.int32, (128, 128), 0)
    lane = lax.broadcasted_iota(jnp.int32, (128, 128), 1)

    total = parts_ref[me % 8]
    landed(got_ref, 0)
    for slot in range(7):
        total = total + got_ref[slot]
    own_ref[...] = total
    one_top[0] = total[:TOP]
    one_low[0] = total[TOP:]

    for slot in order:
        send(own_ref.at[pl.ds(TOP, low)], one_low.at[slot], 1, plane(slot))
    full = unpack_rows(total)
    squared = full * full
    weighed = jnp.where(row > lane, squared + squared, jnp.where(row == lane, squared, 0.0))
    squares = jnp.sum(weighed.reshape(16, 8, 128), axis=0)
    square_own[...] = squares
    for slot in order:
        send(square_own, square_one.at[slot - 1], 2, column(slot))
    for slot in order:
        send(own_ref.at[pl.ds(0, TOP)], one_top.at[slot], 3, column(slot))
    landed(square_one, 2)
    for slot in range(7):
        squares = squares + square_one[slot]
    square_group[...] = squares
    send(square_group, square_side, 4, me, 1 - node)

    landed(one_low.at[pl.ds(1, 7)], 1)
    for slot in range(1, 8):
        send_low[slot - 1] = one_low[low_pick[slot]]
    two_low[0] = one_low[low_pick[0]]
    for slot in order:
        send(send_low.at[slot - 1], two_low.at[slot], 5, column(slot))
    landed(square_side, 4)
    squares = squares + square_side[...]
    square_both[...] = squares
    for slot in order:
        send(square_both, square_two.at[slot - 1], 6, plane(slot))
    landed(one_top.at[pl.ds(1, 7)], 3)
    for slot in range(1, 8):
        send_top[slot - 1] = one_top[top_pick[slot]]
    two_top[0] = one_top[top_pick[0]]
    for slot in order:
        send(send_top.at[slot - 1], two_top.at[slot], 7, plane(slot))

    landed(square_two, 6)
    for slot in range(7):
        squares = squares + square_two[slot]
    squares_ref[...] = squares
    left(got_ref, 0)
    left(send_low, 1)
    left(square_one, 2)
    left(send_top, 3)
    left(square_side, 4)
    left(square_two, 6)
    landed(two_low.at[pl.ds(1, 7)], 5)
    rows_ref[pl.ds(TOP, low)] = two_low[low_take]
    landed(two_top.at[pl.ds(1, 7)], 7)
    rows_ref[pl.ds(0, TOP)] = two_top[top_take]
    left(send_low, 5)
    left(send_top, 7)


def exchange(parts, source):
    low = ROWS - TOP
    f32 = jnp.float32
    vmem = pl.BlockSpec(memory_space=pltpu.VMEM)
    return pl.pallas_call(
        exchange_kernel,
        out_shape=(pltpu.VMEM((ROWS, 128), f32), pltpu.VMEM((8, 128), f32)),
        in_specs=[vmem, pl.BlockSpec(memory_space=pltpu.SMEM)],
        out_specs=(vmem, vmem),
        scratch_shapes=[
            pltpu.VMEM((7, ROWS, 128), f32),
            pltpu.VMEM((ROWS, 128), f32),
            pltpu.VMEM((8, TOP, 128), f32),
            pltpu.VMEM((8, low, 128), f32),
            pltpu.VMEM((7, TOP, 128), f32),
            pltpu.VMEM((7, low, 128), f32),
            pltpu.VMEM((8, TOP, 128), f32),
            pltpu.VMEM((8, low, 128), f32),
            pltpu.VMEM((8, 128), f32),
            pltpu.VMEM((7, 8, 128), f32),
            pltpu.VMEM((8, 128), f32),
            pltpu.VMEM((8, 128), f32),
            pltpu.VMEM((8, 128), f32),
            pltpu.VMEM((7, 8, 128), f32),
            pltpu.SemaphoreType.DMA((8,)),
            pltpu.SemaphoreType.DMA((8,)),
        ],
        compiler_params=pltpu.CompilerParams(
            collective_id=0, has_side_effects=True, vmem_limit_bytes=8 * 2**20
        ),
        name="exchange",
    )(
        pltpu.with_memory_space_constraint(parts, pltpu.VMEM),
        pltpu.with_memory_space_constraint(source, pltpu.SMEM),
    )


def finish_kernel(rows_ref, squares_ref, out_ref):
    row = lax.broadcasted_iota(jnp.int32, (128, 128), 0)
    lane = lax.broadcasted_iota(jnp.int32, (128, 128), 1)
    entries = 2 * 64 * 128 * 128
    factor = lax.rsqrt(jnp.sum(squares_ref[...], keepdims=True) / entries + 1e-06)
    full = unpack_rows(rows_ref[...])
    lower = jnp.where(row >= lane, full, 0.0)
    out_ref[0, 0] = jnp.where(row >= lane, full, lower.T) * factor


def finish(rows, squares):
    vmem = pl.BlockSpec(memory_space=pltpu.VMEM)
    return pl.pallas_call(
        finish_kernel,
        out_shape=jax.ShapeDtypeStruct((1, 1, 128, 128), jnp.float32),
        in_specs=[vmem, vmem],
        out_specs=vmem,
        compiler_params=pltpu.CompilerParams(vmem_limit_bytes=8 * 2**20),
        name="finish",
    )(
        pltpu.with_memory_space_constraint(rows, pltpu.VMEM),
        pltpu.with_memory_space_constraint(squares, pltpu.VMEM),
    )


def body(env_blocks, iso_blocks, joined_sector, owner_map, live_pairs):
    parts, source = local_sums(env_blocks, iso_blocks, joined_sector, owner_map, live_pairs)
    return finish(*exchange(parts, source))


def solution(mesh):
    placed = (
        P("node", "sec", None, None),
        P("node", "sec", None, None),
        P("node", "sec"),
        P("node", None),
        P("node", "sec"),
    )
    return jax.shard_map(
        body, mesh=mesh, in_specs=placed, out_specs=P("node", "sec", None, None), check_vma=False
    )
```

```python
import functools

import jax
import jax.numpy as jnp
from jax import lax
from jax.experimental import pallas as pl
from jax.experimental.pallas import tpu as pltpu
from jax.sharding import PartitionSpec as P

MESH = pl.DeviceIdType.MESH
NODE_SECTORS = 8
CHUNK = 16
PAIRS = CHUNK // 2
DEPTH = PAIRS // 2
ROWS = 72
TOP = 40


def pack_rows(full):
    lane = lax.broadcasted_iota(jnp.int32, (16, 128), 1)
    rows = [full[112:128]]
    for low in range(3):
        high = 6 - low
        width = 16 * (high + 1)
        short = pltpu.roll(full[16 * low : 16 * low + 16], width, 1)
        rows.append(jnp.where(lane < width, full[16 * high : 16 * high + 16], short))
    rows.append(jnp.where(lane[:8] < 64, full[48:56], pltpu.roll(full[56:64], 64, 1)))
    return jnp.concatenate(rows, axis=0)


def unpack_rows(packed):
    blocks = [None] * 8
    blocks[7] = packed[0:16]
    for low in range(3):
        high = 6 - low
        width = 16 * (high + 1)
        both = packed[16 + 16 * low : 32 + 16 * low]
        blocks[high] = both
        blocks[low] = pltpu.roll(both, 128 - width, 1)
    blocks[3] = jnp.concatenate((packed[64:72], pltpu.roll(packed[64:72], 64, 1)), axis=0)
    return jnp.concatenate(blocks, axis=0)


def local_kernel(
    live_ref, sector_hbm, owner_hbm, env_ref, iso_ref,
    sums_0, sums_1, sums_2, sums_3, source_ref,
    sector_ref, owner_ref, env_buf, iso_buf, carry_buf, load_sem, small_sem,
):
    live = live_ref[0, 0]
    turns = 2
    loops = (live + turns * CHUNK - 1) // (turns * CHUNK)
    last = turns * loops - 1
    sums = (sums_0, sums_1, sums_2, sums_3)

    def begin(first, length, sem):
        span = pl.ds(first, length)
        pltpu.make_async_copy(iso_ref.at[0, span], iso_buf.at[span], load_sem.at[sem]).start()
        pltpu.make_async_copy(env_ref.at[0, span], env_buf.at[span], load_sem.at[sem]).start()

    def arrived(length, sem):
        both = iso_buf.at[pl.ds(0, 2 * length)]
        pltpu.make_async_copy(both, both, load_sem.at[sem]).wait()

    def begin_two(i, carry):
        begin(pl.multiple_of((2 * i - 1) * CHUNK, CHUNK), 2 * CHUNK, i)
        return carry

    small = [
        pltpu.make_async_copy(src, dst, small_sem.at[i])
        for i, (src, dst) in enumerate(
            ((sector_hbm, sector_ref), (owner_hbm, owner_ref))
        )
    ]
    for copy in small:
        copy.start()
    begin(0, CHUNK, 0)
    lax.fori_loop(1, (last + 1) // 2, begin_two, 0)
    begin(pl.multiple_of(last * CHUNK, CHUNK), CHUNK, (last + 1) // 2)

    def clear(sector, carry):
        for ref in sums:
            ref[sector] = jnp.zeros((128, 128), jnp.float32)
        return carry

    lax.fori_loop(0, NODE_SECTORS + 1, clear, 0)
    for copy in small:
        copy.wait()
    def invert(sector, carry):
        source_ref[0, owner_ref[0, sector]] = sector
        return carry

    lax.fori_loop(0, owner_ref.shape[1], invert, 0, unroll=8)

    def target(slot):
        counts = jnp.logical_and(slot >= 0, slot < live)
        return jnp.where(counts, lax.rem(sector_ref[0, jnp.maximum(slot, 0)], NODE_SECTORS), NODE_SECTORS)

    def stage(c, place, mxu, register):
        first = c * CHUNK + 2 * (2 * place + mxu)
        none = jnp.zeros((128, 128), jnp.bfloat16)
        top = jnp.concatenate((iso_buf[first], none), axis=1)
        bottom = jnp.concatenate((none, iso_buf[first + 1]), axis=1)
        pltpu.matmul_push_rhs(
            jnp.concatenate((top, bottom), axis=0), staging_register=register, mxu_index=mxu
        )

    def run(z_acc, y_acc):
        def turned(place, mxu):
            z = pltpu.matmul_pop(z_acc[mxu][place]).astype(jnp.bfloat16)
            return jnp.concatenate((z[:, :128].T, z[:, 128:].T), axis=1)

        def first_stage(c, place, mxu, register):
            stage(c, place, mxu, register)
            first = c * CHUNK + 2 * (2 * place + mxu)
            side = jnp.concatenate((env_buf[first], env_buf[first + 1]), axis=1)
            pltpu.matmul_acc_lhs(z_acc[mxu][place], side, load_staged_rhs=register)

        def add(c, place, mxu):
            y = pltpu.matmul_pop(y_acc[mxu][place])
            for half in range(2):
                where = target(c * CHUNK + 2 * (2 * place + mxu) + half)
                ref = sums[2 * mxu + half]
                ref[where] = ref[where] + y[:, 128 * half : 128 * half + 128]

        def second_stage(place, mxu, register, side):
            pltpu.matmul_acc_lhs(y_acc[mxu][place], side, load_staged_rhs=register)

        both = range(2)

        def turn(c, sides):
            for mxu in both:
                add(c - 3, 3, mxu)
                second_stage(3, mxu, 0, sides[mxu])
            ready = []
            for place in range(2):
                ready.append([turned(place, mxu) for mxu in both])
                for mxu in both:
                    first_stage(c, place, mxu, 1 - place)
            for mxu in both:
                add(c - 2, 0, mxu)
                stage(c - 1, 0, mxu, 1)
                second_stage(0, mxu, 1, ready[0][mxu])
            for place in range(2, 4):
                ready.append([turned(place, mxu) for mxu in both])
                for mxu in both:
                    first_stage(c, place, mxu, 0)
                for mxu in both:
                    add(c - 2, place - 1, mxu)
                    stage(c - 1, place - 1, mxu, 1)
                    second_stage(place - 1, mxu, 1, ready[place - 1][mxu])
            for mxu in both:
                stage(c - 1, 3, mxu, 0)
            return ready[3]

        for place in range(DEPTH):
            for mxu in both:
                pltpu.matmul_pop(z_acc[mxu][place])
                pltpu.matmul_pop(y_acc[mxu][place])
        arrived(CHUNK, 0)
        for place in range(DEPTH):
            for mxu in both:
                first_stage(0, place, mxu, place % 2)
        for mxu in both:
            stage(0, 3, mxu, 0)
            carry_buf[mxu] = jnp.zeros((128, 256), jnp.bfloat16)

        def many(step, carry):
            c = turns * step + 1
            arrived(2 * CHUNK, turns // 2 * step + 1)
            sides = [carry_buf[mxu] for mxu in both]
            sides = turn(c, sides)
            sides = turn(c + 1, sides)
            for mxu in both:
                carry_buf[mxu] = sides[mxu]
            return carry

        lax.fori_loop(0, loops - 1, many, 0)
        sides = [carry_buf[mxu] for mxu in both]
        arrived(CHUNK, (last + 1) // 2)
        sides = turn(last, sides)
        drained = [[turned(place, mxu) for mxu in both] for place in range(2)]
        for mxu in both:
            add(last - 2, 3, mxu)
            second_stage(3, mxu, 0, sides[mxu])
        for place in range(2, 4):
            drained.append([turned(place, mxu) for mxu in both])
        for place in range(4):
            for mxu in both:
                add(last - 1, place, mxu)
                stage(last, place, mxu, 1 - place % 2)
                second_stage(place, mxu, 1 - place % 2, drained[place][mxu])
        for place in range(4):
            for mxu in both:
                add(last, place, mxu)

    accs = [[pltpu.ACC(mxu)((128, 256), jnp.float32) for _ in range(DEPTH)] for mxu in range(2)]
    pl.run_scoped(run, accs, accs)


def local_sums(env_blocks, iso_blocks, joined_sector, owner_map, live_pairs):
    pairs = env_blocks.shape[1]
    hbm = pl.BlockSpec(memory_space=pltpu.HBM)
    return pl.pallas_call(
        local_kernel,
        out_shape=(
            *[pltpu.VMEM((NODE_SECTORS + 1, 128, 128), jnp.float32)] * 4,
            pltpu.SMEM(owner_map.shape, jnp.int32),
        ),
        in_specs=[pl.BlockSpec(memory_space=pltpu.SMEM)] + [hbm] * 4,
        out_specs=(*[pl.BlockSpec(memory_space=pltpu.VMEM)] * 4, pl.BlockSpec(memory_space=pltpu.SMEM)),
        scratch_shapes=[
            pltpu.SMEM(joined_sector.shape, jnp.int32),
            pltpu.SMEM(owner_map.shape, jnp.int32),
            pltpu.VMEM((pairs, 128, 128), jnp.bfloat16),
            pltpu.VMEM((pairs, 128, 128), jnp.bfloat16),
            pltpu.VMEM((2, 128, 256), jnp.bfloat16),
            pltpu.SemaphoreType.DMA((pairs // (2 * CHUNK) + 1,)),
            pltpu.SemaphoreType.DMA((2,)),
        ],
        compiler_params=pltpu.CompilerParams(
            vmem_limit_bytes=40 * 2**20,
        ),
        name="local_sums",
    )(live_pairs, *[
        pltpu.with_memory_space_constraint(array, pltpu.HBM)
        for array in (joined_sector, owner_map, env_blocks, iso_blocks)
    ])


def exchange_kernel(
    sums_0, sums_1, sums_2, sums_3, source_ref, rows_ref, squares_ref,
    parts_ref, got_ref, own_ref, one_top, one_low, send_top, send_low, two_top, two_low,
    square_own, square_one, square_group, square_side, square_both, square_two, sent_sem, got_sem,
):
    me = lax.axis_index("sec")
    node = lax.axis_index("node")
    x, y, z = lax.div(me, 16), lax.rem(lax.div(me, 4), 4), lax.rem(me, 4)
    odd = lax.rem(y, 2)
    near = y + 1 - 2 * odd
    far = lax.rem(y + 3 + 2 * odd, 4)
    low = ROWS - TOP
    order = (6, 2, 5, 7, 1, 3, 4)
    row_z = [lax.rem(z + d, 4) for d in range(4)]
    row_x = [lax.rem(x + d, 4) * 16 + z for d in range(4)]
    plane_y = (me - z, me - z + 4 * (near - y))
    column_y = (y * 4, far * 4)
    planes = [plane_y[slot // 4] + row_z[slot % 4] for slot in range(8)]
    columns = [row_x[slot % 4] + column_y[slot // 4] for slot in range(8)]

    def plane(slot):
        return planes[slot]

    def column(slot):
        return columns[slot]

    def send(src, dst, phase, place, group=node):
        pltpu.make_async_remote_copy(
            src_ref=src, dst_ref=dst, send_sem=sent_sem.at[phase], recv_sem=got_sem.at[phase],
            device_id=(place, group), device_id_type=MESH,
        ).start()

    def landed(ref, phase):
        pltpu.make_async_copy(ref, ref, got_sem.at[phase]).wait()

    def left(ref, phase):
        pltpu.make_async_copy(ref, ref, sent_sem.at[phase]).wait()

    barrier = pltpu.get_barrier_semaphore()
    for slot in order:
        pl.semaphore_signal(barrier, inc=1, device_id=(plane(slot), node), device_id_type=MESH)
    for slot in order:
        pl.semaphore_signal(barrier, inc=1, device_id=(column(slot), node), device_id_type=MESH)
    pl.semaphore_signal(barrier, inc=1, device_id=(me, 1 - node), device_id_type=MESH)

    for sector in range(NODE_SECTORS):
        full = (sums_0[sector] + sums_1[sector]) + (sums_2[sector] + sums_3[sector])
        parts_ref[sector] = pack_rows(full)
    pl.semaphore_wait(barrier, 15)

    for slot in order:
        member = lax.rem(plane(slot), 8)
        send(parts_ref.at[member], got_ref.at[slot - 1], 0, plane(slot))

    def cut(source):
        return lax.div(source, 16), lax.rem(lax.div(source, 4), 4), lax.rem(source, 4)

    def back(here, there):
        return lax.rem(here + 4 - there, 4)

    top_pick, low_pick = [], []
    for slot in range(8):
        xs, ys, zs = cut(source_ref[0, plane(slot)])
        top_pick.append(jnp.where(ys == y, 0, 4) + back(x, xs))
        xs, ys, zs = cut(source_ref[0, column(slot)])
        low_pick.append(jnp.where(ys == y, 0, 4) + back(z, zs))
    xs, ys, zs = cut(source_ref[0, me])
    far_s = lax.rem(ys + 3 + 2 * lax.rem(ys, 2), 4)
    same = lax.div(y, 2) == lax.div(ys, 2)
    middle = jnp.where(same, ys, far_s)
    top_take = jnp.where(middle == y, 0, 4) + back(z, zs)
    low_take = jnp.where(same, 0, 4) + back(x, xs)

    row = lax.broadcasted_iota(jnp.int32, (128, 128), 0)
    lane = lax.broadcasted_iota(jnp.int32, (128, 128), 1)

    total = parts_ref[lax.rem(me, 8)]
    landed(got_ref, 0)
    for slot in range(7):
        total = total + got_ref[slot]
    full = unpack_rows(total)
    squared = full * full
    weighed = jnp.where(row > lane, squared + squared, jnp.where(row == lane, squared, 0.0))
    squares = jnp.sum(weighed.reshape(16, 8, 128), axis=0)
    own_ref[...] = total
    square_own[...] = squares
    one_top[0] = total[:TOP]
    one_low[0] = total[TOP:]

    for slot in order:
        send(square_own, square_one.at[slot - 1], 2, plane(slot))
    for slot in order:
        send(own_ref.at[pl.ds(0, TOP)], one_top.at[slot], 3, column(slot))
    for slot in order:
        send(own_ref.at[pl.ds(TOP, low)], one_low.at[slot], 1, plane(slot))
    landed(square_one, 2)
    for slot in range(7):
        squares = squares + square_one[slot]
    square_group[...] = squares
    send(square_group, square_side, 4, me, 1 - node)

    landed(one_top.at[pl.ds(1, 7)], 3)
    for slot in order:
        send_top[slot - 1] = one_top[top_pick[slot]]
    for slot in order:
        send(send_top.at[slot - 1], two_top.at[slot], 7, plane(slot))
    two_top[0] = one_top[top_pick[0]]
    landed(one_low.at[pl.ds(1, 7)], 1)
    for slot in order:
        send_low[slot - 1] = one_low[low_pick[slot]]
    for slot in order:
        send(send_low.at[slot - 1], two_low.at[slot], 5, column(slot))
    two_low[0] = one_low[low_pick[0]]
    landed(square_side, 4)
    squares = squares + square_side[...]
    square_both[...] = squares
    for slot in order:
        send(square_both, square_two.at[slot - 1], 6, column(slot))

    left(got_ref, 0)
    left(send_low, 1)
    left(square_one, 2)
    left(send_top, 3)
    left(square_side, 4)
    landed(square_two, 6)
    for slot in range(7):
        squares = squares + square_two[slot]
    squares_ref[...] = squares
    left(square_two, 6)
    landed(two_top.at[pl.ds(1, 7)], 7)
    rows_ref[pl.ds(0, TOP)] = two_top[top_take]
    landed(two_low.at[pl.ds(1, 7)], 5)
    rows_ref[pl.ds(TOP, low)] = two_low[low_take]
    left(send_low, 5)
    left(send_top, 7)


def exchange(sums, source):
    low = ROWS - TOP
    f32 = jnp.float32
    vmem = pl.BlockSpec(memory_space=pltpu.VMEM)
    return pl.pallas_call(
        exchange_kernel,
        out_shape=(pltpu.VMEM((ROWS, 128), f32), pltpu.VMEM((8, 128), f32)),
        in_specs=[*[vmem] * 4, pl.BlockSpec(memory_space=pltpu.SMEM)],
        out_specs=(vmem, vmem),
        scratch_shapes=[
            pltpu.VMEM((NODE_SECTORS, ROWS, 128), f32),
            pltpu.VMEM((7, ROWS, 128), f32),
            pltpu.VMEM((ROWS, 128), f32),
            pltpu.VMEM((8, TOP, 128), f32),
            pltpu.VMEM((8, low, 128), f32),
            pltpu.VMEM((7, TOP, 128), f32),
            pltpu.VMEM((7, low, 128), f32),
            pltpu.VMEM((8, TOP, 128), f32),
            pltpu.VMEM((8, low, 128), f32),
            pltpu.VMEM((8, 128), f32),
            pltpu.VMEM((7, 8, 128), f32),
            pltpu.VMEM((8, 128), f32),
            pltpu.VMEM((8, 128), f32),
            pltpu.VMEM((8, 128), f32),
            pltpu.VMEM((7, 8, 128), f32),
            pltpu.SemaphoreType.DMA((8,)),
            pltpu.SemaphoreType.DMA((8,)),
        ],
        compiler_params=pltpu.CompilerParams(
            collective_id=0, has_side_effects=True, vmem_limit_bytes=8 * 2**20
        ),
        name="exchange",
    )(
        *[pltpu.with_memory_space_constraint(array, pltpu.VMEM) for array in sums],
        pltpu.with_memory_space_constraint(source, pltpu.SMEM),
    )


def finish_kernel(rows_ref, squares_ref, out_ref):
    row = lax.broadcasted_iota(jnp.int32, (128, 128), 0)
    lane = lax.broadcasted_iota(jnp.int32, (128, 128), 1)
    entries = 2 * 64 * 128 * 128
    factor = lax.rsqrt(jnp.sum(squares_ref[...], keepdims=True) / entries + 1e-06)
    full = unpack_rows(rows_ref[...])
    lower = jnp.where(row >= lane, full, 0.0)
    out_ref[0, 0] = jnp.where(row >= lane, full, lower.T) * factor


def finish(rows, squares):
    vmem = pl.BlockSpec(memory_space=pltpu.VMEM)
    return pl.pallas_call(
        finish_kernel,
        out_shape=jax.ShapeDtypeStruct((1, 1, 128, 128), jnp.float32),
        in_specs=[vmem, vmem],
        out_specs=vmem,
        compiler_params=pltpu.CompilerParams(vmem_limit_bytes=8 * 2**20),
        name="finish",
    )(
        pltpu.with_memory_space_constraint(rows, pltpu.VMEM),
        pltpu.with_memory_space_constraint(squares, pltpu.VMEM),
    )


def body(env_blocks, iso_blocks, joined_sector, owner_map, live_pairs):
    *sums, source = local_sums(env_blocks, iso_blocks, joined_sector, owner_map, live_pairs)
    return finish(*exchange(sums, source))


def solution(mesh):
    placed = (
        P("node", "sec", None, None),
        P("node", "sec", None, None),
        P("node", "sec"),
        P("node", None),
        P("node", "sec"),
    )
    return jax.shard_map(
        body, mesh=mesh, in_specs=placed, out_specs=P("node", "sec", None, None), check_vma=False
    )
```

```python
import functools

import jax
import jax.numpy as jnp
from jax import lax
from jax.experimental import pallas as pl
from jax.experimental.pallas import tpu as pltpu
from jax.sharding import PartitionSpec as P

MESH = pl.DeviceIdType.MESH
NODE_SECTORS = 8
CHUNK = 16
PAIRS = CHUNK // 2
DEPTH = PAIRS // 2
ROWS = 72
TOP = 40


def pack_rows(full):
    lane = lax.broadcasted_iota(jnp.int32, (16, 128), 1)
    rows = [full[112:128]]
    for low in range(3):
        high = 6 - low
        width = 16 * (high + 1)
        short = pltpu.roll(full[16 * low : 16 * low + 16], width, 1)
        rows.append(jnp.where(lane < width, full[16 * high : 16 * high + 16], short))
    rows.append(jnp.where(lane[:8] < 64, full[48:56], pltpu.roll(full[56:64], 64, 1)))
    return jnp.concatenate(rows, axis=0)


def unpack_rows(packed):
    blocks = [None] * 8
    blocks[7] = packed[0:16]
    for low in range(3):
        high = 6 - low
        width = 16 * (high + 1)
        both = packed[16 + 16 * low : 32 + 16 * low]
        blocks[high] = both
        blocks[low] = pltpu.roll(both, 128 - width, 1)
    blocks[3] = jnp.concatenate((packed[64:72], pltpu.roll(packed[64:72], 64, 1)), axis=0)
    return jnp.concatenate(blocks, axis=0)


def local_kernel(
    live_ref, sector_hbm, owner_hbm, env_ref, iso_ref,
    sums_0, sums_1, sums_2, sums_3, source_ref,
    sector_ref, owner_ref, env_buf, iso_buf, carry_buf, load_sem, small_sem,
):
    live = live_ref[0, 0]
    turns = 2
    loops = (live + turns * CHUNK - 1) // (turns * CHUNK)
    last = turns * loops - 1
    sums = (sums_0, sums_1, sums_2, sums_3)

    def begin(first, length, sem):
        span = pl.ds(first, length)
        pltpu.make_async_copy(iso_ref.at[0, span], iso_buf.at[span], load_sem.at[sem]).start()
        pltpu.make_async_copy(env_ref.at[0, span], env_buf.at[span], load_sem.at[sem]).start()

    def arrived(length, sem):
        both = iso_buf.at[pl.ds(0, 2 * length)]
        pltpu.make_async_copy(both, both, load_sem.at[sem]).wait()

    def begin_two(i, carry):
        begin(pl.multiple_of((2 * i - 1) * CHUNK, CHUNK), 2 * CHUNK, i)
        return carry

    small = [
        pltpu.make_async_copy(src, dst, small_sem.at[i])
        for i, (src, dst) in enumerate(
            ((sector_hbm, sector_ref), (owner_hbm, owner_ref))
        )
    ]
    for copy in small:
        copy.start()
    begin(0, CHUNK, 0)
    lax.fori_loop(1, (last + 1) // 2, begin_two, 0)
    begin(pl.multiple_of(last * CHUNK, CHUNK), CHUNK, (last + 1) // 2)

    def clear(sector, carry):
        for ref in sums:
            ref[sector] = jnp.zeros((128, 128), jnp.float32)
        return carry

    lax.fori_loop(0, NODE_SECTORS + 1, clear, 0)
    for copy in small:
        copy.wait()
    def invert(sector, carry):
        source_ref[0, owner_ref[0, sector]] = sector
        return carry

    lax.fori_loop(0, owner_ref.shape[1], invert, 0, unroll=8)

    def target(slot):
        counts = jnp.logical_and(slot >= 0, slot < live)
        return jnp.where(counts, lax.rem(sector_ref[0, jnp.maximum(slot, 0)], NODE_SECTORS), NODE_SECTORS)

    def stage(c, place, mxu, register):
        first = c * CHUNK + 2 * (2 * place + mxu)
        none = jnp.zeros((128, 128), jnp.bfloat16)
        top = jnp.concatenate((iso_buf[first], none), axis=1)
        bottom = jnp.concatenate((none, iso_buf[first + 1]), axis=1)
        pltpu.matmul_push_rhs(
            jnp.concatenate((top, bottom), axis=0), staging_register=register, mxu_index=mxu
        )

    def run(z_acc, y_acc):
        def turned(place, mxu):
            z = pltpu.matmul_pop(z_acc[mxu][place]).astype(jnp.bfloat16)
            return jnp.concatenate((z[:, :128].T, z[:, 128:].T), axis=1)

        def first_stage(c, place, mxu, register):
            stage(c, place, mxu, register)
            first = c * CHUNK + 2 * (2 * place + mxu)
            side = jnp.concatenate((env_buf[first], env_buf[first + 1]), axis=1)
            pltpu.matmul_acc_lhs(z_acc[mxu][place], side, load_staged_rhs=register)

        def add(c, place, mxu):
            y = pltpu.matmul_pop(y_acc[mxu][place])
            for half in range(2):
                where = target(c * CHUNK + 2 * (2 * place + mxu) + half)
                ref = sums[2 * mxu + half]
                ref[where] = ref[where] + y[:, 128 * half : 128 * half + 128]

        def second_stage(place, mxu, register, side):
            pltpu.matmul_acc_lhs(y_acc[mxu][place], side, load_staged_rhs=register)

        both = range(2)

        def turn(c, sides):
            for mxu in both:
                add(c - 3, 3, mxu)
                second_stage(3, mxu, 0, sides[mxu])
            ready = []
            for place in range(2):
                ready.append([turned(place, mxu) for mxu in both])
                for mxu in both:
                    first_stage(c, place, mxu, 1 - place)
            for mxu in both:
                add(c - 2, 0, mxu)
                stage(c - 1, 0, mxu, 1)
                second_stage(0, mxu, 1, ready[0][mxu])
            for place in range(2, 4):
                ready.append([turned(place, mxu) for mxu in both])
                for mxu in both:
                    first_stage(c, place, mxu, 0)
                for mxu in both:
                    add(c - 2, place - 1, mxu)
                    stage(c - 1, place - 1, mxu, 1)
                    second_stage(place - 1, mxu, 1, ready[place - 1][mxu])
            for mxu in both:
                stage(c - 1, 3, mxu, 0)
            return ready[3]

        for place in range(DEPTH):
            for mxu in both:
                pltpu.matmul_pop(z_acc[mxu][place])
                pltpu.matmul_pop(y_acc[mxu][place])
        arrived(CHUNK, 0)
        for place in range(DEPTH):
            for mxu in both:
                first_stage(0, place, mxu, place % 2)
        for mxu in both:
            stage(0, 3, mxu, 0)
            carry_buf[mxu] = jnp.zeros((128, 256), jnp.bfloat16)

        def many(step, carry):
            c = turns * step + 1
            arrived(2 * CHUNK, turns // 2 * step + 1)
            sides = [carry_buf[mxu] for mxu in both]
            sides = turn(c, sides)
            sides = turn(c + 1, sides)
            for mxu in both:
                carry_buf[mxu] = sides[mxu]
            return carry

        lax.fori_loop(0, loops - 1, many, 0)
        sides = [carry_buf[mxu] for mxu in both]
        arrived(CHUNK, (last + 1) // 2)
        sides = turn(last, sides)
        drained = [[turned(place, mxu) for mxu in both] for place in range(2)]
        for mxu in both:
            add(last - 2, 3, mxu)
            second_stage(3, mxu, 0, sides[mxu])
        for place in range(2, 4):
            drained.append([turned(place, mxu) for mxu in both])
        for place in range(4):
            for mxu in both:
                add(last - 1, place, mxu)
                stage(last, place, mxu, 1 - place % 2)
                second_stage(place, mxu, 1 - place % 2, drained[place][mxu])
        for place in range(4):
            for mxu in both:
                add(last, place, mxu)

    accs = [[pltpu.ACC(mxu)((128, 256), jnp.float32) for _ in range(DEPTH)] for mxu in range(2)]
    pl.run_scoped(run, accs, accs)


def local_sums(env_blocks, iso_blocks, joined_sector, owner_map, live_pairs):
    pairs = env_blocks.shape[1]
    hbm = pl.BlockSpec(memory_space=pltpu.HBM)
    return pl.pallas_call(
        local_kernel,
        out_shape=(
            *[pltpu.VMEM((NODE_SECTORS + 1, 128, 128), jnp.float32)] * 4,
            pltpu.SMEM(owner_map.shape, jnp.int32),
        ),
        in_specs=[pl.BlockSpec(memory_space=pltpu.SMEM)] + [hbm] * 4,
        out_specs=(*[pl.BlockSpec(memory_space=pltpu.VMEM)] * 4, pl.BlockSpec(memory_space=pltpu.SMEM)),
        scratch_shapes=[
            pltpu.SMEM(joined_sector.shape, jnp.int32),
            pltpu.SMEM(owner_map.shape, jnp.int32),
            pltpu.VMEM((pairs, 128, 128), jnp.bfloat16),
            pltpu.VMEM((pairs, 128, 128), jnp.bfloat16),
            pltpu.VMEM((2, 128, 256), jnp.bfloat16),
            pltpu.SemaphoreType.DMA((pairs // (2 * CHUNK) + 1,)),
            pltpu.SemaphoreType.DMA((2,)),
        ],
        compiler_params=pltpu.CompilerParams(
            vmem_limit_bytes=40 * 2**20,
        ),
        name="local_sums",
    )(live_pairs, *[
        pltpu.with_memory_space_constraint(array, pltpu.HBM)
        for array in (joined_sector, owner_map, env_blocks, iso_blocks)
    ])


def exchange_kernel(
    sums_0, sums_1, sums_2, sums_3, source_ref, rows_ref, squares_ref,
    parts_ref, got_top, got_low, own_ref, one_top, one_low, send_top, send_low, two_top, two_low,
    square_own, square_one, square_group, square_side, square_both, square_two, sent_sem, got_sem,
):
    me = lax.axis_index("sec")
    node = lax.axis_index("node")
    x, y, z = lax.div(me, 16), lax.rem(lax.div(me, 4), 4), lax.rem(me, 4)
    odd = lax.rem(y, 2)
    near = y + 1 - 2 * odd
    far = lax.rem(y + 3 + 2 * odd, 4)
    low = ROWS - TOP
    order = (6, 2, 5, 7, 1, 3, 4)
    row_z = [lax.rem(z + d, 4) for d in range(4)]
    row_x = [lax.rem(x + d, 4) * 16 + z for d in range(4)]
    plane_y = (me - z, me - z + 4 * (near - y))
    column_y = (y * 4, far * 4)
    planes = [plane_y[slot // 4] + row_z[slot % 4] for slot in range(8)]
    columns = [row_x[slot % 4] + column_y[slot // 4] for slot in range(8)]

    def plane(slot):
        return planes[slot]

    def column(slot):
        return columns[slot]

    def send(src, dst, phase, place, group=node):
        pltpu.make_async_remote_copy(
            src_ref=src, dst_ref=dst, send_sem=sent_sem.at[phase], recv_sem=got_sem.at[phase],
            device_id=(place, group), device_id_type=MESH,
        ).start()

    def landed(ref, phase):
        pltpu.make_async_copy(ref, ref, got_sem.at[phase]).wait()

    def left(ref, phase):
        pltpu.make_async_copy(ref, ref, sent_sem.at[phase]).wait()

    barrier = pltpu.get_barrier_semaphore()
    for slot in order:
        pl.semaphore_signal(barrier, inc=1, device_id=(plane(slot), node), device_id_type=MESH)
    for slot in order:
        pl.semaphore_signal(barrier, inc=1, device_id=(column(slot), node), device_id_type=MESH)
    pl.semaphore_signal(barrier, inc=1, device_id=(me, 1 - node), device_id_type=MESH)

    for sector in range(NODE_SECTORS):
        full = (sums_0[sector] + sums_1[sector]) + (sums_2[sector] + sums_3[sector])
        parts_ref[sector] = pack_rows(full)
    pl.semaphore_wait(barrier, 15)

    members = [lax.rem(plane(slot), 8) for slot in range(8)]
    for slot in order:
        send(parts_ref.at[members[slot], pl.ds(0, TOP)], got_top.at[slot - 1], 0, plane(slot))
    for slot in order:
        send(parts_ref.at[members[slot], pl.ds(TOP, low)], got_low.at[slot - 1], 8, plane(slot))

    def cut(source):
        return lax.div(source, 16), lax.rem(lax.div(source, 4), 4), lax.rem(source, 4)

    def back(here, there):
        return lax.rem(here + 4 - there, 4)

    top_pick, low_pick = [], []
    for slot in range(8):
        xs, ys, zs = cut(source_ref[0, plane(slot)])
        top_pick.append(jnp.where(ys == y, 0, 4) + back(x, xs))
        xs, ys, zs = cut(source_ref[0, column(slot)])
        low_pick.append(jnp.where(ys == y, 0, 4) + back(z, zs))
    xs, ys, zs = cut(source_ref[0, me])
    far_s = lax.rem(ys + 3 + 2 * lax.rem(ys, 2), 4)
    same = lax.div(y, 2) == lax.div(ys, 2)
    middle = jnp.where(same, ys, far_s)
    top_take = jnp.where(middle == y, 0, 4) + back(z, zs)
    low_take = jnp.where(same, 0, 4) + back(x, xs)

    row = lax.broadcasted_iota(jnp.int32, (128, 128), 0)
    lane = lax.broadcasted_iota(jnp.int32, (128, 128), 1)

    upper = parts_ref[members[0], pl.ds(0, TOP)]
    landed(got_top, 0)
    for slot in range(7):
        upper = upper + got_top[slot]
    own_ref[pl.ds(0, TOP)] = upper
    one_top[0] = upper
    for slot in order:
        send(own_ref.at[pl.ds(0, TOP)], one_top.at[slot], 3, column(slot))
    lower = parts_ref[members[0], pl.ds(TOP, low)]
    landed(got_low, 8)
    for slot in range(7):
        lower = lower + got_low[slot]
    full = unpack_rows(jnp.concatenate((upper, lower), axis=0))
    squared = full * full
    weighed = jnp.where(row > lane, squared + squared, jnp.where(row == lane, squared, 0.0))
    squares = jnp.sum(weighed.reshape(16, 8, 128), axis=0)
    own_ref[pl.ds(TOP, low)] = lower
    square_own[...] = squares
    one_low[0] = lower
    for slot in order:
        send(square_own, square_one.at[slot - 1], 2, plane(slot))
    for slot in order:
        send(own_ref.at[pl.ds(TOP, low)], one_low.at[slot], 1, plane(slot))
    landed(square_one, 2)
    for slot in range(7):
        squares = squares + square_one[slot]
    square_group[...] = squares
    send(square_group, square_side, 4, me, 1 - node)

    landed(one_top.at[pl.ds(1, 7)], 3)
    for slot in order:
        send_top[slot - 1] = one_top[top_pick[slot]]
    for slot in order:
        send(send_top.at[slot - 1], two_top.at[slot], 7, plane(slot))
    two_top[0] = one_top[top_pick[0]]
    landed(one_low.at[pl.ds(1, 7)], 1)
    for slot in order:
        send_low[slot - 1] = one_low[low_pick[slot]]
    for slot in order:
        send(send_low.at[slot - 1], two_low.at[slot], 5, column(slot))
    two_low[0] = one_low[low_pick[0]]
    landed(square_side, 4)
    squares = squares + square_side[...]
    square_both[...] = squares
    for slot in order:
        send(square_both, square_two.at[slot - 1], 6, column(slot))

    left(got_top, 0)
    left(got_low, 8)
    left(send_low, 1)
    left(square_one, 2)
    left(send_top, 3)
    left(square_side, 4)
    landed(square_two, 6)
    for slot in range(7):
        squares = squares + square_two[slot]
    squares_ref[...] = squares
    left(square_two, 6)
    landed(two_top.at[pl.ds(1, 7)], 7)
    rows_ref[pl.ds(0, TOP)] = two_top[top_take]
    landed(two_low.at[pl.ds(1, 7)], 5)
    rows_ref[pl.ds(TOP, low)] = two_low[low_take]
    left(send_low, 5)
    left(send_top, 7)


def exchange(sums, source):
    low = ROWS - TOP
    f32 = jnp.float32
    vmem = pl.BlockSpec(memory_space=pltpu.VMEM)
    return pl.pallas_call(
        exchange_kernel,
        out_shape=(pltpu.VMEM((ROWS, 128), f32), pltpu.VMEM((8, 128), f32)),
        in_specs=[*[vmem] * 4, pl.BlockSpec(memory_space=pltpu.SMEM)],
        out_specs=(vmem, vmem),
        scratch_shapes=[
            pltpu.VMEM((NODE_SECTORS, ROWS, 128), f32),
            pltpu.VMEM((7, TOP, 128), f32),
            pltpu.VMEM((7, low, 128), f32),
            pltpu.VMEM((ROWS, 128), f32),
            pltpu.VMEM((8, TOP, 128), f32),
            pltpu.VMEM((8, low, 128), f32),
            pltpu.VMEM((7, TOP, 128), f32),
            pltpu.VMEM((7, low, 128), f32),
            pltpu.VMEM((8, TOP, 128), f32),
            pltpu.VMEM((8, low, 128), f32),
            pltpu.VMEM((8, 128), f32),
            pltpu.VMEM((7, 8, 128), f32),
            pltpu.VMEM((8, 128), f32),
            pltpu.VMEM((8, 128), f32),
            pltpu.VMEM((8, 128), f32),
            pltpu.VMEM((7, 8, 128), f32),
            pltpu.SemaphoreType.DMA((9,)),
            pltpu.SemaphoreType.DMA((9,)),
        ],
        compiler_params=pltpu.CompilerParams(
            collective_id=0, has_side_effects=True, vmem_limit_bytes=8 * 2**20
        ),
        name="exchange",
    )(
        *[pltpu.with_memory_space_constraint(array, pltpu.VMEM) for array in sums],
        pltpu.with_memory_space_constraint(source, pltpu.SMEM),
    )


def finish_kernel(rows_ref, squares_ref, out_ref):
    row = lax.broadcasted_iota(jnp.int32, (128, 128), 0)
    lane = lax.broadcasted_iota(jnp.int32, (128, 128), 1)
    entries = 2 * 64 * 128 * 128
    factor = lax.rsqrt(jnp.sum(squares_ref[...], keepdims=True) / entries + 1e-06)
    full = unpack_rows(rows_ref[...])
    lower = jnp.where(row >= lane, full, 0.0)
    out_ref[0, 0] = jnp.where(row >= lane, full, lower.T) * factor


def finish(rows, squares):
    vmem = pl.BlockSpec(memory_space=pltpu.VMEM)
    return pl.pallas_call(
        finish_kernel,
        out_shape=jax.ShapeDtypeStruct((1, 1, 128, 128), jnp.float32),
        in_specs=[vmem, vmem],
        out_specs=vmem,
        compiler_params=pltpu.CompilerParams(vmem_limit_bytes=8 * 2**20),
        name="finish",
    )(
        pltpu.with_memory_space_constraint(rows, pltpu.VMEM),
        pltpu.with_memory_space_constraint(squares, pltpu.VMEM),
    )


def body(env_blocks, iso_blocks, joined_sector, owner_map, live_pairs):
    *sums, source = local_sums(env_blocks, iso_blocks, joined_sector, owner_map, live_pairs)
    return finish(*exchange(sums, source))


def solution(mesh):
    placed = (
        P("node", "sec", None, None),
        P("node", "sec", None, None),
        P("node", "sec"),
        P("node", None),
        P("node", "sec"),
    )
    return jax.shard_map(
        body, mesh=mesh, in_specs=placed, out_specs=P("node", "sec", None, None), check_vma=False
    )
```

```python
import functools

import jax
import jax.numpy as jnp
from jax import lax
from jax.experimental import pallas as pl
from jax.experimental.pallas import tpu as pltpu
from jax.sharding import PartitionSpec as P

MESH = pl.DeviceIdType.MESH
NODE_SECTORS = 8
CHUNK = 16
PAIRS = CHUNK // 2
DEPTH = PAIRS // 2
ROWS = 72
TOP = 40
SENT = 28


def pack_rows(full):
    lane = lax.broadcasted_iota(jnp.int32, (8, 128), 1)
    tiles = [full[8 * i : 8 * i + 8] for i in range(16)]
    rows = [tiles[15]]
    for low in range(7):
        width = 8 * (15 - low)
        rows.append(jnp.where(lane < width, tiles[14 - low], pltpu.roll(tiles[low], width, 1)))
    rows.append(jnp.where(lane < 64, tiles[7], pltpu.roll(pltpu.roll(tiles[7], 4, 0), 64, 1)))
    return jnp.concatenate(rows, axis=0)


def unpack_rows(packed):
    sublane = lax.broadcasted_iota(jnp.int32, (8, 128), 0)
    tiles = [None] * 16
    tiles[15] = packed[0:8]
    for low in range(7):
        both = packed[8 + 8 * low : 16 + 8 * low]
        tiles[14 - low] = both
        tiles[low] = pltpu.roll(both, 128 - 8 * (15 - low), 1)
    last = packed[64:72]
    tiles[7] = jnp.where(sublane < 4, last, pltpu.roll(pltpu.roll(last, 4, 0), 64, 1))
    return jnp.concatenate(tiles, axis=0)


def local_kernel(
    live_ref, sector_hbm, owner_hbm, env_ref, iso_ref,
    sums_0, sums_1, sums_2, sums_3, source_ref,
    sector_ref, owner_ref, env_buf, iso_buf, carry_buf, load_sem, small_sem,
):
    live = live_ref[0, 0]
    turns = 2
    loops = (live + turns * CHUNK - 1) // (turns * CHUNK)
    last = turns * loops - 1
    sums = (sums_0, sums_1, sums_2, sums_3)

    def begin(first, length, sem):
        span = pl.ds(first, length)
        pltpu.make_async_copy(iso_ref.at[0, span], iso_buf.at[span], load_sem.at[sem]).start()
        pltpu.make_async_copy(env_ref.at[0, span], env_buf.at[span], load_sem.at[sem]).start()

    def arrived(length, sem):
        both = iso_buf.at[pl.ds(0, 2 * length)]
        pltpu.make_async_copy(both, both, load_sem.at[sem]).wait()

    def begin_two(i, carry):
        begin(pl.multiple_of((2 * i - 1) * CHUNK, CHUNK), 2 * CHUNK, i)
        return carry

    small = [
        pltpu.make_async_copy(src, dst, small_sem.at[i])
        for i, (src, dst) in enumerate(
            ((sector_hbm, sector_ref), (owner_hbm, owner_ref))
        )
    ]
    for copy in small:
        copy.start()
    begin(0, CHUNK, 0)
    lax.fori_loop(1, (last + 1) // 2, begin_two, 0)
    begin(pl.multiple_of(last * CHUNK, CHUNK), CHUNK, (last + 1) // 2)

    def clear(sector, carry):
        for ref in sums:
            ref[sector] = jnp.zeros((128, 128), jnp.float32)
        return carry

    lax.fori_loop(0, NODE_SECTORS + 1, clear, 0)
    for copy in small:
        copy.wait()
    def invert(sector, carry):
        source_ref[0, owner_ref[0, sector]] = sector
        return carry

    lax.fori_loop(0, owner_ref.shape[1], invert, 0, unroll=8)

    def target(slot):
        counts = jnp.logical_and(slot >= 0, slot < live)
        return jnp.where(counts, lax.rem(sector_ref[0, jnp.maximum(slot, 0)], NODE_SECTORS), NODE_SECTORS)

    def stage(c, place, mxu, register):
        first = c * CHUNK + 2 * (2 * place + mxu)
        none = jnp.zeros((128, 128), jnp.bfloat16)
        top = jnp.concatenate((iso_buf[first], none), axis=1)
        bottom = jnp.concatenate((none, iso_buf[first + 1]), axis=1)
        pltpu.matmul_push_rhs(
            jnp.concatenate((top, bottom), axis=0), staging_register=register, mxu_index=mxu
        )

    def run(z_acc, y_acc):
        def turned(place, mxu):
            z = pltpu.matmul_pop(z_acc[mxu][place]).astype(jnp.bfloat16)
            return jnp.concatenate((z[:, :128].T, z[:, 128:].T), axis=1)

        def first_stage(c, place, mxu, register):
            stage(c, place, mxu, register)
            first = c * CHUNK + 2 * (2 * place + mxu)
            side = jnp.concatenate((env_buf[first], env_buf[first + 1]), axis=1)
            pltpu.matmul_acc_lhs(z_acc[mxu][place], side, load_staged_rhs=register)

        def add(c, place, mxu):
            y = pltpu.matmul_pop(y_acc[mxu][place])
            for half in range(2):
                where = target(c * CHUNK + 2 * (2 * place + mxu) + half)
                ref = sums[2 * mxu + half]
                ref[where] = ref[where] + y[:, 128 * half : 128 * half + 128]

        def second_stage(place, mxu, register, side):
            pltpu.matmul_acc_lhs(y_acc[mxu][place], side, load_staged_rhs=register)

        both = range(2)

        def turn(c, sides):
            for mxu in both:
                add(c - 3, 3, mxu)
                second_stage(3, mxu, 0, sides[mxu])
            ready = []
            for place in range(2):
                ready.append([turned(place, mxu) for mxu in both])
                for mxu in both:
                    first_stage(c, place, mxu, 1 - place)
            for mxu in both:
                add(c - 2, 0, mxu)
                stage(c - 1, 0, mxu, 1)
                second_stage(0, mxu, 1, ready[0][mxu])
            for place in range(2, 4):
                ready.append([turned(place, mxu) for mxu in both])
                for mxu in both:
                    first_stage(c, place, mxu, 0)
                for mxu in both:
                    add(c - 2, place - 1, mxu)
                    stage(c - 1, place - 1, mxu, 1)
                    second_stage(place - 1, mxu, 1, ready[place - 1][mxu])
            for mxu in both:
                stage(c - 1, 3, mxu, 0)
            return ready[3]

        for place in range(DEPTH):
            for mxu in both:
                pltpu.matmul_pop(z_acc[mxu][place])
                pltpu.matmul_pop(y_acc[mxu][place])
        arrived(CHUNK, 0)
        for place in range(DEPTH):
            for mxu in both:
                first_stage(0, place, mxu, place % 2)
        for mxu in both:
            stage(0, 3, mxu, 0)
            carry_buf[mxu] = jnp.zeros((128, 256), jnp.bfloat16)

        def many(step, carry):
            c = turns * step + 1
            arrived(2 * CHUNK, turns // 2 * step + 1)
            sides = [carry_buf[mxu] for mxu in both]
            sides = turn(c, sides)
            sides = turn(c + 1, sides)
            for mxu in both:
                carry_buf[mxu] = sides[mxu]
            return carry

        lax.fori_loop(0, loops - 1, many, 0)
        sides = [carry_buf[mxu] for mxu in both]
        arrived(CHUNK, (last + 1) // 2)
        sides = turn(last, sides)
        drained = [[turned(place, mxu) for mxu in both] for place in range(2)]
        for mxu in both:
            add(last - 2, 3, mxu)
            second_stage(3, mxu, 0, sides[mxu])
        for place in range(2, 4):
            drained.append([turned(place, mxu) for mxu in both])
        for place in range(4):
            for mxu in both:
                add(last - 1, place, mxu)
                stage(last, place, mxu, 1 - place % 2)
                second_stage(place, mxu, 1 - place % 2, drained[place][mxu])
        for place in range(4):
            for mxu in both:
                add(last, place, mxu)

    accs = [[pltpu.ACC(mxu)((128, 256), jnp.float32) for _ in range(DEPTH)] for mxu in range(2)]
    pl.run_scoped(run, accs, accs)


def local_sums(env_blocks, iso_blocks, joined_sector, owner_map, live_pairs):
    pairs = env_blocks.shape[1]
    hbm = pl.BlockSpec(memory_space=pltpu.HBM)
    return pl.pallas_call(
        local_kernel,
        out_shape=(
            *[pltpu.VMEM((NODE_SECTORS + 1, 128, 128), jnp.float32)] * 4,
            pltpu.SMEM(owner_map.shape, jnp.int32),
        ),
        in_specs=[pl.BlockSpec(memory_space=pltpu.SMEM)] + [hbm] * 4,
        out_specs=(*[pl.BlockSpec(memory_space=pltpu.VMEM)] * 4, pl.BlockSpec(memory_space=pltpu.SMEM)),
        scratch_shapes=[
            pltpu.SMEM(joined_sector.shape, jnp.int32),
            pltpu.SMEM(owner_map.shape, jnp.int32),
            pltpu.VMEM((pairs, 128, 128), jnp.bfloat16),
            pltpu.VMEM((pairs, 128, 128), jnp.bfloat16),
            pltpu.VMEM((2, 128, 256), jnp.bfloat16),
            pltpu.SemaphoreType.DMA((pairs // (2 * CHUNK) + 1,)),
            pltpu.SemaphoreType.DMA((2,)),
        ],
        compiler_params=pltpu.CompilerParams(
            vmem_limit_bytes=40 * 2**20,
        ),
        name="local_sums",
    )(live_pairs, *[
        pltpu.with_memory_space_constraint(array, pltpu.HBM)
        for array in (joined_sector, owner_map, env_blocks, iso_blocks)
    ])


def exchange_kernel(
    sums_0, sums_1, sums_2, sums_3, source_ref, rows_ref, squares_ref,
    parts_ref, got_top, got_low, own_ref, one_top, one_low, send_top, send_low, two_top, two_low,
    square_own, square_one, square_group, square_side, square_both, square_two, sent_sem, got_sem,
):
    me = lax.axis_index("sec")
    node = lax.axis_index("node")
    x, y, z = lax.div(me, 16), lax.rem(lax.div(me, 4), 4), lax.rem(me, 4)
    odd = lax.rem(y, 2)
    near = y + 1 - 2 * odd
    far = lax.rem(y + 3 + 2 * odd, 4)
    low = ROWS - TOP
    order = (6, 2, 5, 7, 1, 3, 4)
    row_z = [lax.rem(z + d, 4) for d in range(4)]
    row_x = [lax.rem(x + d, 4) * 16 + z for d in range(4)]
    plane_y = (me - z, me - z + 4 * (near - y))
    column_y = (y * 4, far * 4)
    planes = [plane_y[slot // 4] + row_z[slot % 4] for slot in range(8)]
    columns = [row_x[slot % 4] + column_y[slot // 4] for slot in range(8)]

    def plane(slot):
        return planes[slot]

    def column(slot):
        return columns[slot]

    def send(src, dst, phase, place, group=node):
        pltpu.make_async_remote_copy(
            src_ref=src, dst_ref=dst, send_sem=sent_sem.at[phase], recv_sem=got_sem.at[phase],
            device_id=(place, group), device_id_type=MESH,
        ).start()

    def landed(ref, phase):
        pltpu.make_async_copy(ref, ref, got_sem.at[phase]).wait()

    def left(ref, phase):
        pltpu.make_async_copy(ref, ref, sent_sem.at[phase]).wait()

    barrier = pltpu.get_barrier_semaphore()
    for slot in order:
        pl.semaphore_signal(barrier, inc=1, device_id=(plane(slot), node), device_id_type=MESH)
    for slot in order:
        pl.semaphore_signal(barrier, inc=1, device_id=(column(slot), node), device_id_type=MESH)
    pl.semaphore_signal(barrier, inc=1, device_id=(me, 1 - node), device_id_type=MESH)

    for sector in range(NODE_SECTORS):
        full = (sums_0[sector] + sums_1[sector]) + (sums_2[sector] + sums_3[sector])
        parts_ref[sector] = pack_rows(full)
    pl.semaphore_wait(barrier, 15)

    members = [lax.rem(plane(slot), 8) for slot in range(8)]
    for slot in order:
        send(parts_ref.at[members[slot], pl.ds(0, TOP)], got_top.at[slot - 1], 0, plane(slot))
    for slot in order:
        send(parts_ref.at[members[slot], pl.ds(TOP, SENT)], got_low.at[slot - 1, pl.ds(0, SENT)], 8, plane(slot))

    def cut(source):
        return lax.div(source, 16), lax.rem(lax.div(source, 4), 4), lax.rem(source, 4)

    def back(here, there):
        return lax.rem(here + 4 - there, 4)

    top_pick, low_pick = [], []
    for slot in range(8):
        xs, ys, zs = cut(source_ref[0, plane(slot)])
        top_pick.append(jnp.where(ys == y, 0, 4) + back(x, xs))
        xs, ys, zs = cut(source_ref[0, column(slot)])
        low_pick.append(jnp.where(ys == y, 0, 4) + back(z, zs))
    xs, ys, zs = cut(source_ref[0, me])
    far_s = lax.rem(ys + 3 + 2 * lax.rem(ys, 2), 4)
    same = lax.div(y, 2) == lax.div(ys, 2)
    middle = jnp.where(same, ys, far_s)
    top_take = jnp.where(middle == y, 0, 4) + back(z, zs)
    low_take = jnp.where(same, 0, 4) + back(x, xs)

    row = lax.broadcasted_iota(jnp.int32, (128, 128), 0)
    lane = lax.broadcasted_iota(jnp.int32, (128, 128), 1)

    upper = parts_ref[members[0], pl.ds(0, TOP)]
    landed(got_top, 0)
    for slot in range(7):
        upper = upper + got_top[slot]
    own_ref[pl.ds(0, TOP)] = upper
    one_top[0] = upper
    for slot in order:
        send(own_ref.at[pl.ds(0, TOP)], one_top.at[slot], 3, column(slot))
    lower = parts_ref[members[0], pl.ds(TOP, low)]
    landed(got_low.at[:, pl.ds(0, SENT)], 8)
    for slot in range(7):
        lower = lower + got_low[slot]
    full = unpack_rows(jnp.concatenate((upper, lower), axis=0))
    squared = full * full
    weighed = jnp.where(row > lane, squared + squared, jnp.where(row == lane, squared, 0.0))
    squares = jnp.sum(weighed.reshape(16, 8, 128), axis=0)
    own_ref[pl.ds(TOP, low)] = lower
    square_own[...] = squares
    one_low[0] = lower
    for slot in order:
        send(square_own, square_one.at[slot - 1], 2, plane(slot))
    for slot in order:
        send(own_ref.at[pl.ds(TOP, SENT)], one_low.at[slot, pl.ds(0, SENT)], 1, plane(slot))
    landed(square_one, 2)
    for slot in range(7):
        squares = squares + square_one[slot]
    square_group[...] = squares
    send(square_group, square_side, 4, me, 1 - node)

    landed(one_top.at[pl.ds(1, 7)], 3)
    for slot in order:
        send_top[slot - 1] = one_top[top_pick[slot]]
    for slot in order:
        send(send_top.at[slot - 1], two_top.at[slot], 7, plane(slot))
    two_top[0] = one_top[top_pick[0]]
    landed(one_low.at[pl.ds(1, 7), pl.ds(0, SENT)], 1)
    for slot in order:
        send_low[slot - 1] = one_low[low_pick[slot]]
    for slot in order:
        send(send_low.at[slot - 1, pl.ds(0, SENT)], two_low.at[slot, pl.ds(0, SENT)], 5, column(slot))
    two_low[0] = one_low[low_pick[0]]
    landed(square_side, 4)
    squares = squares + square_side[...]
    square_both[...] = squares
    for slot in order:
        send(square_both, square_two.at[slot - 1], 6, column(slot))

    left(got_top, 0)
    left(got_low.at[:, pl.ds(0, SENT)], 8)
    left(send_low.at[:, pl.ds(0, SENT)], 1)
    left(square_one, 2)
    left(send_top, 3)
    left(square_side, 4)
    landed(square_two, 6)
    for slot in range(7):
        squares = squares + square_two[slot]
    squares_ref[...] = squares
    left(square_two, 6)
    landed(two_top.at[pl.ds(1, 7)], 7)
    rows_ref[pl.ds(0, TOP)] = two_top[top_take]
    landed(two_low.at[pl.ds(1, 7), pl.ds(0, SENT)], 5)
    rows_ref[pl.ds(TOP, low)] = two_low[low_take]
    left(send_low.at[:, pl.ds(0, SENT)], 5)
    left(send_top, 7)


def exchange(sums, source):
    low = ROWS - TOP
    f32 = jnp.float32
    vmem = pl.BlockSpec(memory_space=pltpu.VMEM)
    return pl.pallas_call(
        exchange_kernel,
        out_shape=(pltpu.VMEM((ROWS, 128), f32), pltpu.VMEM((8, 128), f32)),
        in_specs=[*[vmem] * 4, pl.BlockSpec(memory_space=pltpu.SMEM)],
        out_specs=(vmem, vmem),
        scratch_shapes=[
            pltpu.VMEM((NODE_SECTORS, ROWS, 128), f32),
            pltpu.VMEM((7, TOP, 128), f32),
            pltpu.VMEM((7, low, 128), f32),
            pltpu.VMEM((ROWS, 128), f32),
            pltpu.VMEM((8, TOP, 128), f32),
            pltpu.VMEM((8, low, 128), f32),
            pltpu.VMEM((7, TOP, 128), f32),
            pltpu.VMEM((7, low, 128), f32),
            pltpu.VMEM((8, TOP, 128), f32),
            pltpu.VMEM((8, low, 128), f32),
            pltpu.VMEM((8, 128), f32),
            pltpu.VMEM((7, 8, 128), f32),
            pltpu.VMEM((8, 128), f32),
            pltpu.VMEM((8, 128), f32),
            pltpu.VMEM((8, 128), f32),
            pltpu.VMEM((7, 8, 128), f32),
            pltpu.SemaphoreType.DMA((9,)),
            pltpu.SemaphoreType.DMA((9,)),
        ],
        compiler_params=pltpu.CompilerParams(
            collective_id=0, has_side_effects=True, vmem_limit_bytes=8 * 2**20
        ),
        name="exchange",
    )(
        *[pltpu.with_memory_space_constraint(array, pltpu.VMEM) for array in sums],
        pltpu.with_memory_space_constraint(source, pltpu.SMEM),
    )


def finish_kernel(rows_ref, squares_ref, out_ref):
    row = lax.broadcasted_iota(jnp.int32, (128, 128), 0)
    lane = lax.broadcasted_iota(jnp.int32, (128, 128), 1)
    entries = 2 * 64 * 128 * 128
    factor = lax.rsqrt(jnp.sum(squares_ref[...], keepdims=True) / entries + 1e-06)
    full = unpack_rows(rows_ref[...])
    lower = jnp.where(row >= lane, full, 0.0)
    out_ref[0, 0] = jnp.where(row >= lane, full, lower.T) * factor


def finish(rows, squares):
    vmem = pl.BlockSpec(memory_space=pltpu.VMEM)
    return pl.pallas_call(
        finish_kernel,
        out_shape=jax.ShapeDtypeStruct((1, 1, 128, 128), jnp.float32),
        in_specs=[vmem, vmem],
        out_specs=vmem,
        compiler_params=pltpu.CompilerParams(vmem_limit_bytes=8 * 2**20),
        name="finish",
    )(
        pltpu.with_memory_space_constraint(rows, pltpu.VMEM),
        pltpu.with_memory_space_constraint(squares, pltpu.VMEM),
    )


def body(env_blocks, iso_blocks, joined_sector, owner_map, live_pairs):
    *sums, source = local_sums(env_blocks, iso_blocks, joined_sector, owner_map, live_pairs)
    return finish(*exchange(sums, source))


def solution(mesh):
    placed = (
        P("node", "sec", None, None),
        P("node", "sec", None, None),
        P("node", "sec"),
        P("node", None),
        P("node", "sec"),
    )
    return jax.shard_map(
        body, mesh=mesh, in_specs=placed, out_specs=P("node", "sec", None, None), check_vma=False
    )
```
